32 devices in a mesh: tile: 8 (over z, y), grp: 4 (over x, core).
Axes of the slice: x: 2, y: 2, z: 4, core: 2. Of those that a mesh axis runs over, the one named last changes fastest.
Arguments:
- basis: float32 [16384, 2401], P(('tile', 'grp')), may hold values from -6 to 6
- pixel_ids: int32 [262144], P(('tile', 'grp')), may hold values from 0 to 511
- band_ids: int32 [262144], P(('tile', 'grp')), may hold values from 0 to 4
- mags: float32 [262144], P(('tile', 'grp')), may hold values from -6 to 6
- inv_var: float32 [262144], P(('tile', 'grp')), may hold values from 0.01 to 10
Outputs:
- solution: float32 [5, 2401], replicated
- residual: float32 [5, 2401], replicated
The draws below stay inside these ranges and needn't reach their ends.
All inputs are finite; a program needn't handle non-finite values.
Results may differ from the reference program's by a relative error of at most 0.0003.
Values sent between devices are 32-bit elements; how exact they have to be, the bound alone decides.
A program may use at most 64 MiB of HBM per device.

```python
import math
import jax
import jax.numpy as jnp
from jax import lax

BANDS = 5
NCOEF = 2401
PIX_DEV = 512
OBJ_DEV = 8192
ITERS = 3
PIXELS = 16384
OBJECTS = 262144


def touch_ends(entries, rng, least, top_value):
    extent = entries.shape
    place = [jax.random.randint(jax.random.fold_in(rng, axis), (), 0, extent[axis]) for axis in range(len(extent))]
    entries = entries.at[tuple(place)].set(least)
    longest = extent.index(max(extent))
    place[longest] = (place[longest] + 1) % extent[longest]
    return entries.at[tuple(place)].set(top_value)


def block_levels(key, dims, cuts, low, largest):
    def one(position, parts):
        steps = jax.random.uniform(jax.random.fold_in(jax.random.fold_in(key, 6), position), (parts,), jnp.float32, low / len(cuts), largest / len(cuts))
        return jnp.repeat(jnp.exp(steps), dims[position] // parts).reshape((-1,) + (1,) * (len(dims) - position - 1))

    factor_of = one(*cuts[0])
    for cut in cuts[1:]:
        factor_of = factor_of * one(*cut)
    return factor_of


def centred(stream_key, dims, scale, limit, cuts=(), kind=jnp.bfloat16):
    level = block_levels(stream_key, dims, cuts, -0.22, 0.18) if cuts else 1.0
    entries = jax.random.normal(stream_key, dims, jnp.float32) * scale * level
    return jnp.minimum(jnp.maximum(entries, -limit), limit).astype(kind)


def setup_inputs(seed: int = 0) -> dict:
    key_list = jax.random.split(jax.random.key(seed), 6)
    basis = centred(key_list[0], (PIXELS, NCOEF), 1.0, 6.0, ((0, 32),), jnp.float32)
    pixel_ids = touch_ends(jax.random.randint(key_list[1], (OBJECTS,), 0, PIX_DEV), jax.random.fold_in(key_list[1], 1), 0, PIX_DEV - 1).astype(jnp.int32)
    band_ids = touch_ends(jax.random.randint(key_list[2], (OBJECTS,), 0, BANDS), jax.random.fold_in(key_list[2], 1), 0, BANDS - 1).astype(jnp.int32)
    mags = centred(key_list[3], (OBJECTS,), 1.0, 6.0, ((0, 32),), jnp.float32)
    inv_var = jnp.clip(jnp.exp(math.log(10.0) - 6.9077553 * jax.random.uniform(key_list[4], (OBJECTS,), jnp.float32) ** block_levels(key_list[4], (OBJECTS,), ((0, 32),), -0.2, 0.2)), 0.01, 10.0)
    return {"basis": basis, "pixel_ids": pixel_ids, "band_ids": band_ids, "mags": mags, "inv_var": inv_var}


ridge = 0.1

def reference(basis, pixel_ids, band_ids, mags, inv_var):
    total = basis.shape[0]
    rows = pixel_ids.shape[0]
    owner = jnp.arange(rows, dtype=jnp.int32) // OBJ_DEV * PIX_DEV
    segment = (band_ids * total + pixel_ids + owner).astype(jnp.int32)
    counts = jax.ops.segment_sum(inv_var, segment, num_segments=BANDS * total).reshape(BANDS, total)
    weighted = jax.ops.segment_sum(inv_var * mags, segment, num_segments=BANDS * total).reshape(BANDS, total)
    block = math.gcd(total, 32768)
    nblocks = total // block
    blocks = basis.reshape(nblocks, block, NCOEF)
    count_blocks = jnp.transpose(counts.reshape(BANDS, nblocks, block), (1, 0, 2))
    weight_blocks = jnp.transpose(weighted.reshape(BANDS, nblocks, block), (1, 0, 2))

    def rhs_step(acc, pieces):
        tiles, weights = pieces
        return (acc + jnp.dot(weights, tiles, precision=lax.Precision.HIGHEST), None)
    zero = jnp.zeros((BANDS, NCOEF), jnp.float32)
    local_rhs, _ = lax.scan(rhs_step, zero, (blocks, weight_blocks))
    right_side = local_rhs / jnp.sqrt(jnp.float32(total))

    def apply_op(direction):

        def op_step(acc, pieces):
            tiles, cnt = pieces
            model = jnp.dot(direction, tiles.T, precision=lax.Precision.HIGHEST)
            scaled = cnt * model
            return (acc + jnp.dot(scaled, tiles, precision=lax.Precision.HIGHEST), None)
        summed, _ = lax.scan(op_step, zero, (blocks, count_blocks))
        return summed / jnp.float32(total) + ridge * direction
    solution = zero
    residual = right_side
    direction = right_side
    norm_now = jnp.sum(residual * residual)
    for step in range(ITERS):
        image = apply_op(direction)
        step_len = norm_now / jnp.sum(direction * image)
        solution = solution + step_len * direction
        residual = residual - step_len * image
        norm_next = jnp.sum(residual * residual)
        direction = residual + norm_next / norm_now * direction
        norm_now = norm_next
    return (solution, residual)
```

```python
import functools

import jax
import jax.numpy as jnp
from jax import lax
from jax.experimental import pallas as pl
from jax.experimental.pallas import tpu as pltpu
from jax.sharding import PartitionSpec as P

BANDS = 5
ITERS = 3
RIDGE = 0.1
STEPS = ITERS + 1
LANES = 128
F32 = jnp.float32
BF16 = jnp.bfloat16
MESH = pl.DeviceIdType.MESH

UNROLL = 64
MIDDLE = 4
SKIP = 2
ODD = 1
SUB = 16
GROUPS = 2


def split_rows(value):
    high = value.astype(BF16).astype(F32)
    return jnp.concatenate([high, value - high], axis=0).astype(BF16)


def fold(value):
    return value[:8] + value[8:]


def tree(terms):
    while len(terms) > 1:
        terms = [
            terms[i] + terms[i + 1] if i + 1 < len(terms) else terms[i]
            for i in range(0, len(terms), 2)
        ]
    return terms[0]


class Plan:
    def __init__(self, tsize, gsize, ncoef):
        self.tsize, self.gsize, self.ndev = tsize, gsize, tsize * gsize
        whole = tsize % MIDDLE == 0
        self.t0, self.tcount = (tsize // MIDDLE, tsize // 2) if whole else (0, tsize)
        self.skip, self.odd = (SKIP, ODD) if gsize % SKIP == 0 else (1, 0)
        self.per_tile = gsize // self.skip
        self.side = self.tcount * self.per_tile // 2
        self.ktiles = -(-ncoef // LANES)
        self.ht = -(-self.ktiles // 2)
        self.ht += -self.ht % GROUPS
        self.gt = self.ht // GROUPS
        self.nh = min(self.side, self.ht)
        self.pieces = [(j * self.ht // self.nh, (j + 1) * self.ht // self.nh) for j in range(self.nh)]
        self.sizes = sorted({b - a for a, b in self.pieces})
        self.largest = max(self.sizes)
        self.width = 2 * self.ht * LANES


def kernel(
    cfg,
    basis_hbm, pid_hbm, bid_hbm, mag_hbm, ivar_hbm,
    out_ref,
    bas, pid, bid, mag, ivar,
    bhi, blo, cnt, wgt,
    snd, rsb, agb,
    in_sems, send_sems, rs_sems, ag_sems,
):
    pixels, ncoef, objs, plan = cfg
    ht, gt, nh = plan.ht, plan.gt, plan.nh
    ndev, tsize, gsize = plan.ndev, plan.tsize, plan.gsize
    total_pix = pixels * ndev
    hrows = ht * LANES
    grows = gt * LANES

    tile = lax.axis_index("tile")
    grp = lax.axis_index("grp")
    me = tile * gsize + grp
    inside = (tile >= plan.t0) & (tile < plan.t0 + plan.tcount) & (lax.rem(grp, plan.skip) == plan.odd)
    k = (tile - plan.t0) * plan.per_tile + grp // plan.skip
    my_half = k // plan.side
    my_piece = k - my_half * plan.side
    is_owner = inside & (my_piece < nh)
    low = tile < tsize // 2
    near = jnp.where(low, 0, 1)
    far = 1 - near

    def at(t, g):
        return {"tile": t, "grp": g}

    def owner_place(h, j):
        o = h * plan.side + j
        return plan.t0 + o // plan.per_tile, lax.rem(o, plan.per_tile) * plan.skip + plan.odd

    barrier = pltpu.get_barrier_semaphore()

    def everyone(send):
        shifts = sorted(range(tsize), key=lambda a: abs(a - tsize // 2))
        turns = sorted(range(gsize), key=lambda b: (b + 1) % 2)
        if ndev - 1 <= UNROLL:
            for a in shifts:
                for b in turns:
                    if a or b:
                        send(lax.rem(tile + a, tsize), lax.rem(grp + b, gsize))
        else:
            def some(i, _):
                a = lax.rem(i // gsize + tsize // 2, tsize)
                b = lax.rem(i, gsize)

                @pl.when(i != (tsize - tsize // 2) * gsize)
                def _():
                    send(lax.rem(tile + a, tsize), lax.rem(grp + b, gsize))
                return 0

            lax.fori_loop(0, ndev, some, 0)

    @pl.when(is_owner)
    def _():
        everyone(
            lambda t, g: pl.semaphore_signal(barrier, inc=1, device_id=at(t, g), device_id_type=MESH)
        )

    small = []
    for i, (src, dst) in enumerate(((pid_hbm, pid), (bid_hbm, bid), (mag_hbm, mag), (ivar_hbm, ivar))):
        c = pltpu.make_async_copy(src, dst, in_sems.at[i])
        c.start()
        small.append(c)

    chunks = []
    for c in range(2 * GROUPS):
        a, z = c * grows, min((c + 1) * grows, ncoef)
        rows = pl.ds(a, z - a)
        chunks.append((a, z, pltpu.make_async_copy(basis_hbm.at[rows, :], bas.at[rows, :], in_sems.at[4 + c])))
    low_order = list(range(GROUPS, 2 * GROUPS)) + list(range(GROUPS))
    high_order = list(range(2 * GROUPS))

    @pl.when(low)
    def _():
        for c in low_order:
            chunks[c][2].start()

    @pl.when(jnp.logical_not(low))
    def _():
        for c in high_order:
            chunks[c][2].start()

    cnt[...] = jnp.zeros_like(cnt)
    wgt[...] = jnp.zeros_like(wgt)
    agb[...] = jnp.zeros_like(agb)

    for c in small:
        c.wait()
    blocks = pixels // LANES
    keys = -(-BANDS * blocks // 8) * 8
    orow = objs // LANES
    step_rows = 8 if orow % 8 == 0 else 1

    def hist_step(i, acc):
        lhs_parts, rhs_parts = [], []
        for r in range(step_rows):
            here = pl.ds(i * step_rows + r, 1)
            pix = pid[here, :]
            key = bid[here, :] * blocks + pix // LANES
            lane = lax.rem(pix, LANES)
            weight = ivar[here, :]
            wmag = weight * mag[here, :]
            hot = lax.broadcasted_iota(jnp.int32, (LANES, LANES), 0) == lane
            rhs_parts.append(jnp.where(hot, F32(1), F32(0)).astype(BF16))
            sel = lax.broadcasted_iota(jnp.int32, (keys, LANES), 0) == key
            w_hi = weight.astype(BF16).astype(F32)
            m_hi = wmag.astype(BF16).astype(F32)
            pieces = [w_hi, weight - w_hi, m_hi, wmag - m_hi]
            lhs_parts.append(
                jnp.concatenate([jnp.where(sel, x, F32(0)) for x in pieces], axis=0).astype(BF16)
            )
        lhs = jnp.concatenate(lhs_parts, axis=1)
        rhs = jnp.concatenate(rhs_parts, axis=1)
        return acc + lax.dot_general(
            lhs, rhs, (((1,), (1,)), ((), ())), preferred_element_type=F32
        )

    acc = lax.fori_loop(0, orow // step_rows, hist_step, jnp.zeros((4 * keys, LANES), F32))
    csum = acc[:keys] + acc[keys : 2 * keys]
    wsum = acc[2 * keys : 3 * keys] + acc[3 * keys :]
    for b in range(BANDS):
        for j in range(blocks):
            r = b * blocks + j
            cnt[b : b + 1, j * LANES : (j + 1) * LANES] = csum[r : r + 1]
            wgt[b : b + 1, j * LANES : (j + 1) * LANES] = wsum[r : r + 1]

    def halve(rows, x):
        h = x.astype(BF16)
        bhi[rows, :] = h
        blo[rows, :] = (x - h.astype(F32)).astype(BF16)

    def halve_rows(a, z):
        full = (z - a) // SUB
        group = max(g for g in range(1, 9) if full % g == 0) * SUB

        @pl.loop(0, full * SUB // group)
        def _(i):
            rows = pl.ds(pl.multiple_of(a + i * group, SUB), group)
            halve(rows, bas[rows, :])

        done = a + full * SUB
        if done < z:
            pad = jnp.zeros((SUB - (z - done), pixels), F32)
            halve(slice(done, done + SUB), jnp.concatenate([bas[done:z, :], pad], axis=0))

    for z in range(-(-ncoef // SUB) * SUB, plan.width, SUB):
        halve(slice(z, z + SUB), jnp.zeros((SUB, pixels), F32))

    def to_coef(s, lhs, base, first, count):
        dims = (((1,), (1,)), ((), ()))
        for a in range(0, count, 2):
            n = min(2, count - a)
            start = (first + a) * LANES
            if not isinstance(start, int):
                start = pl.multiple_of(start, LANES)
            rows = pl.ds(start, n * LANES)
            part = fold(
                lax.dot_general(lhs, bhi[rows, :], dims, preferred_element_type=F32)
                + lax.dot_general(lhs, blo[rows, :], dims, preferred_element_type=F32)
            )
            for i in range(n):
                snd[s, base + a + i] = part[:, i * LANES : (i + 1) * LANES]

    def send_pieces(s, h, pieces):
        for j, (a, z) in pieces:
            t, g = owner_place(h, j)

            @pl.when(jnp.logical_not((t == tile) & (g == grp)))
            def _():
                pltpu.make_async_remote_copy(
                    src_ref=snd.at[s, pl.ds(h * ht + a, z - a), pl.ds(0, BANDS)],
                    dst_ref=rsb.at[s, me, pl.ds(0, z - a), pl.ds(0, BANDS)],
                    send_sem=send_sems.at[s, 0], recv_sem=rs_sems.at[s],
                    device_id=at(t, g), device_id_type=MESH,
                ).start()

    every_piece = list(enumerate(plan.pieces))

    def landed(part, sem):
        pltpu.make_async_copy(part, part, sem).wait()

    def produce(s, scaled):
        lhs = split_rows(scaled)
        for h in (far, near):
            to_coef(s, lhs, h * ht, h * ht, ht)
            send_pieces(s, h, every_piece)

    def own(s):
        for n in plan.sizes:
            first = my_piece * ht // nh
            size = (my_piece + 1) * ht // nh - first

            @pl.when(is_owner & (size == n))
            def _():
                mine = pl.ds(my_half * ht + first, n)
                rsb[s, me, :n] = snd[s, mine]
                landed(rsb.at[s, pl.ds(0, ndev - 1), pl.ds(0, n), pl.ds(0, BANDS)], rs_sems.at[s])
                for i in range(n):
                    agb[s, my_half * ht + first + i, :BANDS] = tree(
                        [rsb[s, d, i, :BANDS] for d in range(ndev)]
                    )
                spread = agb.at[s, mine, pl.ds(0, BANDS)]
                group = first // gt

                def forward(t, g):
                    pltpu.make_async_remote_copy(
                        src_ref=spread, dst_ref=spread,
                        send_sem=send_sems.at[s, 1], recv_sem=ag_sems.at[s, my_half, group],
                        device_id=at(t, g), device_id_type=MESH,
                    ).start()

                everyone(forward)

    def group_wait(s, h, g):
        def part(m):
            return agb.at[s, pl.ds(0, m), pl.ds(0, BANDS)]

        sem = ag_sems.at[s, h, g]
        first = my_piece * ht // nh
        size = (my_piece + 1) * ht // nh - first
        holds = is_owner & (my_half == h) & (first // gt == g)

        @pl.when(jnp.logical_not(holds))
        def _():
            landed(part(gt), sem)

        for n in plan.sizes:
            if n < gt:
                @pl.when(holds & (size == n))
                def _():
                    landed(part(gt - n), sem)

    def consume(s, project):
        halves, pix = [], []
        for h in (near, far):
            tiles = []
            for g in range(GROUPS):
                group_wait(s, h, g)
                here = jnp.concatenate([agb[s, h * ht + g * gt + i] for i in range(gt)], axis=1)
                tiles.append(here)
                if project:
                    lhs = split_rows(here)
                    rows = pl.ds(pl.multiple_of((h * GROUPS + g) * grows, LANES), grows)
                    pix.append(
                        jnp.dot(lhs, bhi[rows, :], preferred_element_type=F32)
                        + jnp.dot(lhs, blo[rows, :], preferred_element_type=F32)
                    )
            halves.append(jnp.concatenate(tiles, axis=1))
        total = None
        if project:
            for part in pix:
                total = part if total is None else total + part
            total = fold(total)
        return halves, total

    def dot_all(xs, ys):
        both = sum(jnp.sum(x * y, axis=0, keepdims=True) for x, y in zip(xs, ys))
        return jnp.sum(both, axis=1, keepdims=True)

    right_lhs = split_rows(wgt[...])

    def opening(order):
        for i, c in enumerate(order):
            a, z, copy = chunks[c]
            h = c // GROUPS
            copy.wait()
            halve_rows(a, z)
            to_coef(0, right_lhs, c * gt, c * gt, gt)
            if i == 0:
                pl.semaphore_wait(barrier, waited)
            first = (c % GROUPS) * gt
            send_pieces(0, h, [(j, p) for j, p in every_piece if first < p[1] <= first + gt])

    waited = jnp.where(is_owner, 2 * nh - 1, 2 * nh)

    @pl.when(low)
    def _():
        opening(low_order)

    @pl.when(jnp.logical_not(low))
    def _():
        opening(high_order)

    own(0)
    sums, seen = consume(0, True)
    root = jnp.sqrt(F32(total_pix))
    residual = [x / root for x in sums]
    pix_res = seen / root
    direction, pix_dir = residual, pix_res
    answer = [jnp.zeros_like(x) for x in residual]
    norm_now = dot_all(residual, residual)
    for it in range(ITERS):
        last = it + 1 == ITERS
        produce(it + 1, cnt[...] * pix_dir)
        own(it + 1)
        sums, seen = consume(it + 1, not last)
        image = [x / F32(total_pix) + RIDGE * d for x, d in zip(sums, direction)]
        step_len = norm_now / dot_all(direction, image)
        answer = [x + step_len * d for x, d in zip(answer, direction)]
        residual = [x - step_len * y for x, y in zip(residual, image)]
        if not last:
            pix_image = seen / F32(total_pix) + RIDGE * pix_dir
            pix_res = pix_res - step_len * pix_image
            norm_next = dot_all(residual, residual)
            rate = norm_next / norm_now
            direction = [x + rate * d for x, d in zip(residual, direction)]
            pix_dir = pix_res + rate * pix_dir
            norm_now = norm_next

    def ordered(pair):
        return jnp.concatenate(
            [jnp.where(low, pair[0], pair[1]), jnp.where(low, pair[1], pair[0])], axis=1
        )

    out_ref[0] = ordered(answer)[:BANDS, :ncoef]
    out_ref[1] = ordered(residual)[:BANDS, :ncoef]

    first = my_piece * ht // nh
    size = (my_piece + 1) * ht // nh - first
    for n in plan.sizes:
        @pl.when(is_owner & (size == n))
        def _():
            for s in range(STEPS):
                landed(snd.at[s, pl.ds(0, 2 * ht - n), pl.ds(0, BANDS)], send_sems.at[s, 0])
                landed(rsb.at[s, pl.ds(0, ndev - 1), pl.ds(0, n), pl.ds(0, BANDS)], send_sems.at[s, 1])

    @pl.when(jnp.logical_not(is_owner))
    def _():
        for s in range(STEPS):
            landed(snd.at[s, pl.ds(0, 2 * ht), pl.ds(0, BANDS)], send_sems.at[s, 0])


def body(basis, pixel_ids, band_ids, mags, inv_var):
    pixels, ncoef = basis.shape
    objs = pixel_ids.shape[0]
    plan = Plan(lax.axis_size("tile"), lax.axis_size("grp"), ncoef)
    cfg = (pixels, ncoef, objs, plan)
    fold_objs = lambda x: x.reshape(objs // LANES, LANES)
    anyspec = pl.BlockSpec(memory_space=pl.ANY)
    out = jax.ShapeDtypeStruct((2, BANDS, ncoef), F32)
    orow = objs // LANES
    both = pl.pallas_call(
        functools.partial(kernel, cfg),
        out_shape=out,
        in_specs=[anyspec] * 5,
        out_specs=pl.BlockSpec(memory_space=pltpu.VMEM),
        scratch_shapes=[
            pltpu.VMEM((ncoef, pixels), F32),
            pltpu.VMEM((orow, LANES), jnp.int32),
            pltpu.VMEM((orow, LANES), jnp.int32),
            pltpu.VMEM((orow, LANES), F32),
            pltpu.VMEM((orow, LANES), F32),
            pltpu.VMEM((plan.width, pixels), BF16),
            pltpu.VMEM((plan.width, pixels), BF16),
            pltpu.VMEM((8, pixels), F32),
            pltpu.VMEM((8, pixels), F32),
            pltpu.VMEM((STEPS, 2 * plan.ht, 8, LANES), F32),
            pltpu.VMEM((STEPS, plan.ndev, plan.largest, 8, LANES), F32),
            pltpu.VMEM((STEPS, 2 * plan.ht, 8, LANES), F32),
            pltpu.SemaphoreType.DMA((4 + 2 * GROUPS,)),
            pltpu.SemaphoreType.DMA((STEPS, 2)),
            pltpu.SemaphoreType.DMA((STEPS,)),
            pltpu.SemaphoreType.DMA((STEPS, 2, GROUPS)),
        ],
        compiler_params=pltpu.CompilerParams(collective_id=0, has_side_effects=True),
    )(basis.T, fold_objs(pixel_ids), fold_objs(band_ids), fold_objs(mags), fold_objs(inv_var))
    return both[0], both[1]


def solution(mesh):
    placed = (
        P(("tile", "grp"), None),
        P(("tile", "grp")),
        P(("tile", "grp")),
        P(("tile", "grp")),
        P(("tile", "grp")),
    )
    return jax.shard_map(body, mesh=mesh, in_specs=placed, out_specs=(P(), P()), check_vma=False)
```

```python
import functools

import jax
import jax.numpy as jnp
from jax import lax
from jax.experimental import pallas as pl
from jax.experimental.pallas import tpu as pltpu
from jax.sharding import PartitionSpec as P

BANDS = 5
ITERS = 3
RIDGE = 0.1
STEPS = ITERS + 1
LANES = 128
F32 = jnp.float32
BF16 = jnp.bfloat16
F8 = jnp.float8_e4m3fn
SHIFT = 1024.0
MESH = pl.DeviceIdType.MESH

UNROLL = 64
MIDDLE = 4
SKIP = 2
ODD = 1
SUB = 32
GROUPS = 2


def split_rows(value):
    high = value.astype(BF16).astype(F32)
    both = jnp.concatenate([high, value - high], axis=0)
    return both.astype(BF16), (both * (1 / SHIFT)).astype(BF16)


def fold(value):
    return value[:8] + value[8:]


def tree(terms):
    while len(terms) > 1:
        terms = [
            terms[i] + terms[i + 1] if i + 1 < len(terms) else terms[i]
            for i in range(0, len(terms), 2)
        ]
    return terms[0]


class Plan:
    def __init__(self, tsize, gsize, ncoef):
        self.tsize, self.gsize, self.ndev = tsize, gsize, tsize * gsize
        whole = tsize % MIDDLE == 0
        self.t0, self.tcount = (tsize // MIDDLE, tsize // 2) if whole else (0, tsize)
        self.skip, self.odd = (SKIP, ODD) if gsize % SKIP == 0 else (1, 0)
        self.per_tile = gsize // self.skip
        self.side = self.tcount * self.per_tile // 2
        self.ktiles = -(-ncoef // LANES)
        self.ht = -(-self.ktiles // 2)
        self.ht += -self.ht % GROUPS
        self.gt = self.ht // GROUPS
        self.nh = min(self.side, self.ht)
        self.pieces = [(j * self.ht // self.nh, (j + 1) * self.ht // self.nh) for j in range(self.nh)]
        self.sizes = sorted({b - a for a, b in self.pieces})
        self.largest = max(self.sizes)
        self.width = 2 * self.ht * LANES


def kernel(
    cfg,
    basis_hbm, pid_hbm, bid_hbm, mag_hbm, ivar_hbm,
    out_ref,
    bas, pid, bid, mag, ivar,
    bhi, blo, thi, tlo, cnt, wgt,
    snd, rsb, agb,
    in_sems, send_sems, rs_sems, ag_sems,
):
    pixels, ncoef, objs, plan = cfg
    ht, gt, nh = plan.ht, plan.gt, plan.nh
    ndev, tsize, gsize = plan.ndev, plan.tsize, plan.gsize
    total_pix = pixels * ndev
    hrows = ht * LANES
    grows = gt * LANES

    tile = lax.axis_index("tile")
    grp = lax.axis_index("grp")
    me = tile * gsize + grp
    inside = (tile >= plan.t0) & (tile < plan.t0 + plan.tcount) & (lax.rem(grp, plan.skip) == plan.odd)
    k = (tile - plan.t0) * plan.per_tile + grp // plan.skip
    my_half = k // plan.side
    my_piece = k - my_half * plan.side
    is_owner = inside & (my_piece < nh)
    low = tile < tsize // 2
    near = jnp.where(low, 0, 1)
    far = 1 - near

    def at(t, g):
        return {"tile": t, "grp": g}

    def owner_place(h, j):
        o = h * plan.side + j
        return plan.t0 + o // plan.per_tile, lax.rem(o, plan.per_tile) * plan.skip + plan.odd

    barrier = pltpu.get_barrier_semaphore()

    def everyone(send):
        shifts = sorted(range(tsize), key=lambda a: abs(a - tsize // 2))
        turns = sorted(range(gsize), key=lambda b: (b + 1) % 2)
        if ndev - 1 <= UNROLL:
            for a in shifts:
                for b in turns:
                    if a or b:
                        send(lax.rem(tile + a, tsize), lax.rem(grp + b, gsize))
        else:
            def some(i, _):
                a = lax.rem(i // gsize + tsize // 2, tsize)
                b = lax.rem(i, gsize)

                @pl.when(i != (tsize - tsize // 2) * gsize)
                def _():
                    send(lax.rem(tile + a, tsize), lax.rem(grp + b, gsize))
                return 0

            lax.fori_loop(0, ndev, some, 0)

    @pl.when(is_owner)
    def _():
        everyone(
            lambda t, g: pl.semaphore_signal(barrier, inc=1, device_id=at(t, g), device_id_type=MESH)
        )

    small = []
    for i, (src, dst) in enumerate(((pid_hbm, pid), (bid_hbm, bid), (mag_hbm, mag), (ivar_hbm, ivar))):
        c = pltpu.make_async_copy(src, dst, in_sems.at[i])
        c.start()
        small.append(c)

    chunks = []
    for c in range(2 * GROUPS):
        a, z = c * grows, min((c + 1) * grows, ncoef)
        rows = pl.ds(a, z - a)
        chunks.append((a, z, pltpu.make_async_copy(basis_hbm.at[rows, :], bas.at[rows, :], in_sems.at[4 + c])))
    low_order = list(range(GROUPS, 2 * GROUPS)) + list(range(GROUPS))
    high_order = list(range(2 * GROUPS))

    @pl.when(low)
    def _():
        for c in low_order:
            chunks[c][2].start()

    @pl.when(jnp.logical_not(low))
    def _():
        for c in high_order:
            chunks[c][2].start()

    cnt[...] = jnp.zeros_like(cnt)
    wgt[...] = jnp.zeros_like(wgt)
    agb[...] = jnp.zeros_like(agb)

    for c in small:
        c.wait()
    blocks = pixels // LANES
    keys = -(-BANDS * blocks // 8) * 8
    orow = objs // LANES
    step_rows = 8 if orow % 8 == 0 else 1

    def hist_step(i, acc):
        lhs_parts, rhs_parts = [], []
        for r in range(step_rows):
            here = pl.ds(i * step_rows + r, 1)
            pix = pid[here, :]
            key = bid[here, :] * blocks + pix // LANES
            lane = lax.rem(pix, LANES)
            weight = ivar[here, :]
            wmag = weight * mag[here, :]
            hot = lax.broadcasted_iota(jnp.int32, (LANES, LANES), 0) == lane
            rhs_parts.append(jnp.where(hot, F32(1), F32(0)).astype(F8))
            sel = lax.broadcasted_iota(jnp.int32, (keys, LANES), 0) == key
            w_hi = weight.astype(BF16).astype(F32)
            m_hi = wmag.astype(BF16).astype(F32)
            pieces = [w_hi, weight - w_hi, m_hi, wmag - m_hi]
            lhs_parts.append(
                jnp.concatenate([jnp.where(sel, x, F32(0)) for x in pieces], axis=0).astype(BF16)
            )
        lhs = jnp.concatenate(lhs_parts, axis=1)
        rhs = jnp.concatenate(rhs_parts, axis=1)
        return acc + lax.dot_general(
            lhs, rhs, (((1,), (1,)), ((), ())), preferred_element_type=F32
        )

    acc = lax.fori_loop(0, orow // step_rows, hist_step, jnp.zeros((4 * keys, LANES), F32))
    csum = acc[:keys] + acc[keys : 2 * keys]
    wsum = acc[2 * keys : 3 * keys] + acc[3 * keys :]
    for b in range(BANDS):
        for j in range(blocks):
            r = b * blocks + j
            cnt[b : b + 1, j * LANES : (j + 1) * LANES] = csum[r : r + 1]
            wgt[b : b + 1, j * LANES : (j + 1) * LANES] = wsum[r : r + 1]

    def halve(rows, x):
        h = x.astype(BF16)
        bhi[rows, :] = h
        blo[rows, :] = ((x - h.astype(F32)) * SHIFT).astype(F8)

    def halve_rows(a, z):
        full = (z - a) // SUB
        group = max(g for g in range(1, 9) if full % g == 0) * SUB

        @pl.loop(0, full * SUB // group)
        def _(i):
            rows = pl.ds(pl.multiple_of(a + i * group, SUB), group)
            halve(rows, bas[rows, :])

        done = a + full * SUB
        if done < z:
            pad = jnp.zeros((SUB - (z - done), pixels), F32)
            halve(slice(done, done + SUB), jnp.concatenate([bas[done:z, :], pad], axis=0))

    for z in range(-(-ncoef // SUB) * SUB, plan.width, SUB):
        halve(slice(z, z + SUB), jnp.zeros((SUB, pixels), F32))

    def to_coef(s, lhs, base, first, count):
        dims = (((1,), (1,)), ((), ()))
        for a in range(0, count, 2):
            n = min(2, count - a)
            start = (first + a) * LANES
            if not isinstance(start, int):
                start = pl.multiple_of(start, LANES)
            rows = pl.ds(start, n * LANES)
            part = fold(
                lax.dot_general(lhs[0], bhi[rows, :], dims, preferred_element_type=F32)
                + lax.dot_general(lhs[1], blo[rows, :], dims, preferred_element_type=F32)
            )
            for i in range(n):
                snd[s, base + a + i] = part[:, i * LANES : (i + 1) * LANES]

    def send_pieces(s, h, pieces):
        for j, (a, z) in pieces:
            t, g = owner_place(h, j)

            @pl.when(jnp.logical_not((t == tile) & (g == grp)))
            def _():
                pltpu.make_async_remote_copy(
                    src_ref=snd.at[s, pl.ds(h * ht + a, z - a), pl.ds(0, BANDS)],
                    dst_ref=rsb.at[s, me, pl.ds(0, z - a), pl.ds(0, BANDS)],
                    send_sem=send_sems.at[s, 0], recv_sem=rs_sems.at[s],
                    device_id=at(t, g), device_id_type=MESH,
                ).start()

    every_piece = list(enumerate(plan.pieces))

    def landed(part, sem):
        pltpu.make_async_copy(part, part, sem).wait()

    def turn_basis():
        @pl.loop(0, 2 * ht)
        def _(i):
            rows = pl.ds(pl.multiple_of(i * LANES, LANES), LANES)
            for c in range(0, pixels, LANES):
                thi[c : c + LANES, rows] = bhi[rows, c : c + LANES].T
                tlo[c : c + LANES, rows] = blo[rows, c : c + LANES].T

    def produce(s, scaled):
        lhs = split_rows(scaled)
        for h in (far, near):
            for a in range(0, ht, 2):
                n = min(2, ht - a)
                cols = pl.ds(pl.multiple_of((h * ht + a) * LANES, LANES), n * LANES)
                part = fold(
                    jnp.dot(lhs[0], thi[:, cols], preferred_element_type=F32)
                    + jnp.dot(lhs[1], tlo[:, cols], preferred_element_type=F32)
                )
                for i in range(n):
                    snd[s, h * ht + a + i] = part[:, i * LANES : (i + 1) * LANES]
            send_pieces(s, h, every_piece)

    def own(s):
        for n in plan.sizes:
            first = my_piece * ht // nh
            size = (my_piece + 1) * ht // nh - first

            @pl.when(is_owner & (size == n))
            def _():
                mine = pl.ds(my_half * ht + first, n)
                rsb[s, me, :n] = snd[s, mine]
                landed(rsb.at[s, pl.ds(0, ndev - 1), pl.ds(0, n), pl.ds(0, BANDS)], rs_sems.at[s])
                for i in range(n):
                    agb[s, my_half * ht + first + i, :BANDS] = tree(
                        [rsb[s, d, i, :BANDS] for d in range(ndev)]
                    )
                spread = agb.at[s, mine, pl.ds(0, BANDS)]
                group = first // gt

                def forward(t, g):
                    pltpu.make_async_remote_copy(
                        src_ref=spread, dst_ref=spread,
                        send_sem=send_sems.at[s, 1], recv_sem=ag_sems.at[s, my_half, group],
                        device_id=at(t, g), device_id_type=MESH,
                    ).start()

                everyone(forward)

    def group_wait(s, h, g):
        def part(m):
            return agb.at[s, pl.ds(0, m), pl.ds(0, BANDS)]

        sem = ag_sems.at[s, h, g]
        first = my_piece * ht // nh
        size = (my_piece + 1) * ht // nh - first
        holds = is_owner & (my_half == h) & (first // gt == g)

        @pl.when(jnp.logical_not(holds))
        def _():
            landed(part(gt), sem)

        for n in plan.sizes:
            if n < gt:
                @pl.when(holds & (size == n))
                def _():
                    landed(part(gt - n), sem)

    def consume(s, project):
        halves, pix = [], []
        for h in (near, far):
            tiles = []
            for g in range(GROUPS):
                group_wait(s, h, g)
                here = jnp.concatenate([agb[s, h * ht + g * gt + i] for i in range(gt)], axis=1)
                tiles.append(here)
                if project:
                    lhs = split_rows(here)
                    rows = pl.ds(pl.multiple_of((h * GROUPS + g) * grows, LANES), grows)
                    pix.append(
                        jnp.dot(lhs[0], bhi[rows, :], preferred_element_type=F32)
                        + jnp.dot(lhs[1], blo[rows, :], preferred_element_type=F32)
                    )
            halves.append(jnp.concatenate(tiles, axis=1))
        total = None
        if project:
            for part in pix:
                total = part if total is None else total + part
            total = fold(total)
        return halves, total

    def dot_all(xs, ys):
        both = sum(jnp.sum(x * y, axis=0, keepdims=True) for x, y in zip(xs, ys))
        return jnp.sum(both, axis=1, keepdims=True)

    right_lhs = split_rows(wgt[...])

    def opening(order):
        for i, c in enumerate(order):
            a, z, copy = chunks[c]
            h = c // GROUPS
            copy.wait()
            halve_rows(a, z)
            to_coef(0, right_lhs, c * gt, c * gt, gt)
            if i == 0:
                pl.semaphore_wait(barrier, waited)
            first = (c % GROUPS) * gt
            send_pieces(0, h, [(j, p) for j, p in every_piece if first < p[1] <= first + gt])

    waited = jnp.where(is_owner, 2 * nh - 1, 2 * nh)

    @pl.when(low)
    def _():
        opening(low_order)

    @pl.when(jnp.logical_not(low))
    def _():
        opening(high_order)

    turn_basis()
    own(0)
    sums, seen = consume(0, True)
    root = jnp.sqrt(F32(total_pix))
    residual = [x / root for x in sums]
    pix_res = seen / root
    direction, pix_dir = residual, pix_res
    answer = [jnp.zeros_like(x) for x in residual]
    norm_now = dot_all(residual, residual)
    for it in range(ITERS):
        last = it + 1 == ITERS
        produce(it + 1, cnt[...] * pix_dir)
        own(it + 1)
        sums, seen = consume(it + 1, not last)
        image = [x / F32(total_pix) + RIDGE * d for x, d in zip(sums, direction)]
        step_len = norm_now / dot_all(direction, image)
        answer = [x + step_len * d for x, d in zip(answer, direction)]
        residual = [x - step_len * y for x, y in zip(residual, image)]
        if not last:
            pix_image = seen / F32(total_pix) + RIDGE * pix_dir
            pix_res = pix_res - step_len * pix_image
            norm_next = dot_all(residual, residual)
            rate = norm_next / norm_now
            direction = [x + rate * d for x, d in zip(residual, direction)]
            pix_dir = pix_res + rate * pix_dir
            norm_now = norm_next

    def ordered(pair):
        return jnp.concatenate(
            [jnp.where(low, pair[0], pair[1]), jnp.where(low, pair[1], pair[0])], axis=1
        )

    out_ref[0] = ordered(answer)[:BANDS, :ncoef]
    out_ref[1] = ordered(residual)[:BANDS, :ncoef]

    first = my_piece * ht // nh
    size = (my_piece + 1) * ht // nh - first
    for n in plan.sizes:
        @pl.when(is_owner & (size == n))
        def _():
            for s in range(STEPS):
                landed(snd.at[s, pl.ds(0, 2 * ht - n), pl.ds(0, BANDS)], send_sems.at[s, 0])
                landed(rsb.at[s, pl.ds(0, ndev - 1), pl.ds(0, n), pl.ds(0, BANDS)], send_sems.at[s, 1])

    @pl.when(jnp.logical_not(is_owner))
    def _():
        for s in range(STEPS):
            landed(snd.at[s, pl.ds(0, 2 * ht), pl.ds(0, BANDS)], send_sems.at[s, 0])


def body(basis, pixel_ids, band_ids, mags, inv_var):
    pixels, ncoef = basis.shape
    objs = pixel_ids.shape[0]
    plan = Plan(lax.axis_size("tile"), lax.axis_size("grp"), ncoef)
    cfg = (pixels, ncoef, objs, plan)
    fold_objs = lambda x: x.reshape(objs // LANES, LANES)
    anyspec = pl.BlockSpec(memory_space=pl.ANY)
    out = jax.ShapeDtypeStruct((2, BANDS, ncoef), F32)
    orow = objs // LANES
    both = pl.pallas_call(
        functools.partial(kernel, cfg),
        out_shape=out,
        in_specs=[anyspec] * 5,
        out_specs=pl.BlockSpec(memory_space=pltpu.VMEM),
        scratch_shapes=[
            pltpu.VMEM((ncoef, pixels), F32),
            pltpu.VMEM((orow, LANES), jnp.int32),
            pltpu.VMEM((orow, LANES), jnp.int32),
            pltpu.VMEM((orow, LANES), F32),
            pltpu.VMEM((orow, LANES), F32),
            pltpu.VMEM((plan.width, pixels), BF16),
            pltpu.VMEM((plan.width, pixels), F8),
            pltpu.VMEM((pixels, plan.width), BF16),
            pltpu.VMEM((pixels, plan.width), F8),
            pltpu.VMEM((8, pixels), F32),
            pltpu.VMEM((8, pixels), F32),
            pltpu.VMEM((STEPS, 2 * plan.ht, 8, LANES), F32),
            pltpu.VMEM((STEPS, plan.ndev, plan.largest, 8, LANES), F32),
            pltpu.VMEM((STEPS, 2 * plan.ht, 8, LANES), F32),
            pltpu.SemaphoreType.DMA((4 + 2 * GROUPS,)),
            pltpu.SemaphoreType.DMA((STEPS, 2)),
            pltpu.SemaphoreType.DMA((STEPS,)),
            pltpu.SemaphoreType.DMA((STEPS, 2, GROUPS)),
        ],
        compiler_params=pltpu.CompilerParams(collective_id=0, has_side_effects=True),
    )(basis.T, fold_objs(pixel_ids), fold_objs(band_ids), fold_objs(mags), fold_objs(inv_var))
    return both[0], both[1]


def solution(mesh):
    placed = (
        P(("tile", "grp"), None),
        P(("tile", "grp")),
        P(("tile", "grp")),
        P(("tile", "grp")),
        P(("tile", "grp")),
    )
    return jax.shard_map(body, mesh=mesh, in_specs=placed, out_specs=(P(), P()), check_vma=False)
```

```python
import functools

import jax
import jax.numpy as jnp
from jax import lax
from jax.experimental import pallas as pl
from jax.experimental.pallas import tpu as pltpu
from jax.sharding import PartitionSpec as P

BANDS = 5
ITERS = 3
RIDGE = 0.1
STEPS = ITERS + 1
LANES = 128
F32 = jnp.float32
BF16 = jnp.bfloat16
F8 = jnp.float8_e4m3fn
SHIFT = 1024.0
MESH = pl.DeviceIdType.MESH

UNROLL = 64
MIDDLE = 4
SKIP = 2
ODD = 1
SUB = 32
GROUPS = 2


def split_rows(value):
    high = value.astype(BF16).astype(F32)
    both = jnp.concatenate([high, value - high], axis=0)
    return both.astype(BF16), (both * (1 / SHIFT)).astype(BF16)


def fold(value):
    return value[:8] + value[8:]


def tree(terms):
    while len(terms) > 1:
        terms = [
            terms[i] + terms[i + 1] if i + 1 < len(terms) else terms[i]
            for i in range(0, len(terms), 2)
        ]
    return terms[0]


class Plan:
    def __init__(self, tsize, gsize, ncoef):
        self.tsize, self.gsize, self.ndev = tsize, gsize, tsize * gsize
        whole = tsize % MIDDLE == 0
        self.t0, self.tcount = (tsize // MIDDLE, tsize // 2) if whole else (0, tsize)
        self.skip, self.odd = (SKIP, ODD) if gsize % SKIP == 0 else (1, 0)
        self.per_tile = gsize // self.skip
        self.side = self.tcount * self.per_tile // 2
        self.ktiles = -(-ncoef // LANES)
        self.ht = -(-self.ktiles // 2)
        self.ht += -self.ht % GROUPS
        self.gt = self.ht // GROUPS
        self.nh = min(self.side, self.ht)
        self.pieces = [(j * self.ht // self.nh, (j + 1) * self.ht // self.nh) for j in range(self.nh)]
        self.sizes = sorted({b - a for a, b in self.pieces})
        self.largest = max(self.sizes)
        self.width = 2 * self.ht * LANES


def kernel(
    cfg,
    basis_hbm, pid_hbm, bid_hbm, mag_hbm, ivar_hbm,
    out_ref,
    bas, pid, bid, mag, ivar,
    bhi, blo, thi, tlo, cnt, wgt,
    snd, loc, rsb, agb,
    in_sems, send_sems, rs_sems, ag_sems,
):
    pixels, ncoef, objs, plan = cfg
    ht, gt, nh = plan.ht, plan.gt, plan.nh
    ndev, tsize, gsize = plan.ndev, plan.tsize, plan.gsize
    total_pix = pixels * ndev
    hrows = ht * LANES
    grows = gt * LANES

    tile = lax.axis_index("tile")
    grp = lax.axis_index("grp")
    me = tile * gsize + grp
    inside = (tile >= plan.t0) & (tile < plan.t0 + plan.tcount) & (lax.rem(grp, plan.skip) == plan.odd)
    k = (tile - plan.t0) * plan.per_tile + grp // plan.skip
    my_half = k // plan.side
    my_piece = k - my_half * plan.side
    is_owner = inside & (my_piece < nh)
    low = tile < tsize // 2
    near = jnp.where(low, 0, 1)
    far = 1 - near

    def at(t, g):
        return {"tile": t, "grp": g}

    def owner_place(h, j):
        o = h * plan.side + j
        return plan.t0 + o // plan.per_tile, lax.rem(o, plan.per_tile) * plan.skip + plan.odd

    barrier = pltpu.get_barrier_semaphore()

    def steps(n, shift):
        return min(shift, n - shift)

    def reach(move):
        a, b = move
        outer, inner = (a // 2, a % 2) if tsize % 2 == 0 else (a, 0)
        return -(
            steps(max(tsize // 2, 1), outer) + inner
            + steps(max(gsize // 2, 1), (b + 1) // 2 % max(gsize // 2, 1)) + (b % 2) * 0.95
        )

    def toward(a, b):
        g = lax.rem(grp + b, gsize)
        if tsize % 2:
            return lax.rem(tile + a, tsize), g
        outer = lax.rem(tile // 2 + a // 2, tsize // 2)
        return outer * 2 + lax.rem(tile + a % 2, 2), g

    def everyone(send):
        moves = sorted(((a, b) for a in range(tsize) for b in range(gsize) if a or b), key=reach)
        if ndev - 1 <= UNROLL:
            for a, b in moves:
                send(*toward(a, b))
        else:
            def some(i, _):
                a = lax.rem(i // gsize + tsize // 2, tsize)
                b = lax.rem(i, gsize)

                @pl.when(i != (tsize - tsize // 2) * gsize)
                def _():
                    send(lax.rem(tile + a, tsize), lax.rem(grp + b, gsize))
                return 0

            lax.fori_loop(0, ndev, some, 0)

    @pl.when(is_owner)
    def _():
        everyone(
            lambda t, g: pl.semaphore_signal(barrier, inc=1, device_id=at(t, g), device_id_type=MESH)
        )

    small = []
    for i, (src, dst) in enumerate(((pid_hbm, pid), (bid_hbm, bid), (mag_hbm, mag), (ivar_hbm, ivar))):
        c = pltpu.make_async_copy(src, dst, in_sems.at[i])
        c.start()
        small.append(c)

    chunks = []
    for c in range(2 * GROUPS):
        a, z = c * grows, min((c + 1) * grows, ncoef)
        rows = pl.ds(a, z - a)
        chunks.append((a, z, pltpu.make_async_copy(basis_hbm.at[rows, :], bas.at[rows, :], in_sems.at[4 + c])))
    low_order = list(range(GROUPS, 2 * GROUPS)) + list(range(GROUPS))
    high_order = list(range(2 * GROUPS))

    @pl.when(low)
    def _():
        for c in low_order:
            chunks[c][2].start()

    @pl.when(jnp.logical_not(low))
    def _():
        for c in high_order:
            chunks[c][2].start()

    cnt[...] = jnp.zeros_like(cnt)
    wgt[...] = jnp.zeros_like(wgt)
    agb[...] = jnp.zeros_like(agb)

    for c in small:
        c.wait()
    blocks = pixels // LANES
    keys = -(-BANDS * blocks // 8) * 8
    orow = objs // LANES
    step_rows = 8 if orow % 8 == 0 else 1

    def histogram(dst, value_of):
        def hist_step(i, acc):
            lhs_parts, rhs_parts = [], []
            for r in range(step_rows):
                here = pl.ds(i * step_rows + r, 1)
                pix = pid[here, :]
                key = bid[here, :] * blocks + pix // LANES
                lane = lax.rem(pix, LANES)
                hot = lax.broadcasted_iota(jnp.int32, (LANES, LANES), 0) == lane
                rhs_parts.append(jnp.where(hot, F32(1), F32(0)).astype(F8))
                sel = lax.broadcasted_iota(jnp.int32, (keys, LANES), 0) == key
                value = value_of(here)
                high = value.astype(BF16).astype(F32)
                lhs_parts.append(
                    jnp.concatenate(
                        [jnp.where(sel, x, F32(0)) for x in (high, value - high)], axis=0
                    ).astype(BF16)
                )
            lhs = jnp.concatenate(lhs_parts, axis=1)
            rhs = jnp.concatenate(rhs_parts, axis=1)
            return acc + lax.dot_general(
                lhs, rhs, (((1,), (1,)), ((), ())), preferred_element_type=F32
            )

        acc = lax.fori_loop(
            0, orow // step_rows, hist_step, jnp.zeros((2 * keys, LANES), F32), unroll=4
        )
        both = acc[:keys] + acc[keys:]
        for b in range(BANDS):
            for j in range(blocks):
                r = b * blocks + j
                dst[b : b + 1, j * LANES : (j + 1) * LANES] = both[r : r + 1]

    histogram(wgt, lambda here: ivar[here, :] * mag[here, :])

    def halve(rows, x):
        h = x.astype(BF16)
        bhi[rows, :] = h
        blo[rows, :] = ((x - h.astype(F32)) * SHIFT).astype(F8)

    def halve_rows(a, z):
        full = (z - a) // SUB

        for i in range(a, a + full * SUB, SUB):
            halve(slice(i, i + SUB), bas[i : i + SUB, :])

        done = a + full * SUB
        if done < z:
            pad = jnp.zeros((SUB - (z - done), pixels), F32)
            halve(slice(done, done + SUB), jnp.concatenate([bas[done:z, :], pad], axis=0))

    for z in range(-(-ncoef // SUB) * SUB, plan.width, SUB):
        halve(slice(z, z + SUB), jnp.zeros((SUB, pixels), F32))

    def to_coef(s, lhs, base, first, count):
        dims = (((1,), (1,)), ((), ()))
        for a in range(0, count, 2):
            n = min(2, count - a)
            start = (first + a) * LANES
            if not isinstance(start, int):
                start = pl.multiple_of(start, LANES)
            rows = pl.ds(start, n * LANES)
            part = fold(
                lax.dot_general(lhs[0], bhi[rows, :], dims, preferred_element_type=F32)
                + lax.dot_general(lhs[1], blo[rows, :], dims, preferred_element_type=F32)
            )
            for i in range(n):
                snd[s, base + a + i] = part[:, i * LANES : (i + 1) * LANES]

    def send_pieces(s, h, pieces):
        for j, (a, z) in pieces:
            t, g = owner_place(h, j)

            @pl.when(jnp.logical_not((t == tile) & (g == grp)))
            def _():
                pltpu.make_async_remote_copy(
                    src_ref=snd.at[s, pl.ds(h * ht + a, z - a), pl.ds(0, BANDS)],
                    dst_ref=rsb.at[s, me, pl.ds(0, z - a), pl.ds(0, BANDS)],
                    send_sem=send_sems.at[s, 0], recv_sem=rs_sems.at[s],
                    device_id=at(t, g), device_id_type=MESH,
                ).start()

    every_piece = list(enumerate(plan.pieces))

    def landed(part, sem):
        pltpu.make_async_copy(part, part, sem).wait()

    def turn_basis():
        @pl.loop(0, 2 * ht)
        def _(i):
            rows = pl.ds(pl.multiple_of(i * LANES, LANES), LANES)
            for c in range(0, pixels, LANES):
                thi[c : c + LANES, rows] = bhi[rows, c : c + LANES].T
                tlo[c : c + LANES, rows] = blo[rows, c : c + LANES].T

    def produce(s, scaled, settle):
        lhs = split_rows(scaled)
        for h in (far, near):
            for a in range(0, ht, 2):
                n = min(2, ht - a)
                cols = pl.ds(pl.multiple_of((h * ht + a) * LANES, LANES), n * LANES)
                part = fold(
                    jnp.dot(lhs[0], thi[:, cols], preferred_element_type=F32)
                    + jnp.dot(lhs[1], tlo[:, cols], preferred_element_type=F32)
                )
                for i in range(n):
                    settle(h * ht + a + i, part[:, i * LANES : (i + 1) * LANES])
            send_pieces(s, h, every_piece)

    def own(s):
        for n in plan.sizes:
            first = my_piece * ht // nh
            size = (my_piece + 1) * ht // nh - first

            @pl.when(is_owner & (size == n))
            def _():
                mine = pl.ds(my_half * ht + first, n)
                rsb[s, me, :n] = snd[s, mine]
                landed(rsb.at[s, pl.ds(0, ndev - 1), pl.ds(0, n), pl.ds(0, BANDS)], rs_sems.at[s])
                for i in range(n):
                    agb[s, my_half * ht + first + i, :BANDS] = tree(
                        [rsb[s, d, i, :BANDS] for d in range(ndev)]
                    )
                spread = agb.at[s, mine, pl.ds(0, BANDS)]
                group = first // gt

                def forward(t, g):
                    pltpu.make_async_remote_copy(
                        src_ref=spread, dst_ref=spread,
                        send_sem=send_sems.at[s, 1], recv_sem=ag_sems.at[s, my_half, group],
                        device_id=at(t, g), device_id_type=MESH,
                    ).start()

                everyone(forward)

    def group_wait(s, h, g):
        def part(m):
            return agb.at[s, pl.ds(0, m), pl.ds(0, BANDS)]

        sem = ag_sems.at[s, h, g]
        first = my_piece * ht // nh
        size = (my_piece + 1) * ht // nh - first
        holds = is_owner & (my_half == h) & (first // gt == g)

        @pl.when(jnp.logical_not(holds))
        def _():
            landed(part(gt), sem)

        for n in plan.sizes:
            if n < gt:
                @pl.when(holds & (size == n))
                def _():
                    landed(part(gt - n), sem)

    def consume(s, project):
        halves, pix = [], []
        for h in (near, far):
            tiles = []
            for g in range(GROUPS):
                group_wait(s, h, g)
                here = jnp.concatenate([agb[s, h * ht + g * gt + i] for i in range(gt)], axis=1)
                tiles.append(here)
                if project:
                    lhs = split_rows(here)
                    rows = pl.ds(pl.multiple_of((h * GROUPS + g) * grows, LANES), grows)
                    pix.append(
                        jnp.dot(lhs[0], bhi[rows, :], preferred_element_type=F32)
                        + jnp.dot(lhs[1], blo[rows, :], preferred_element_type=F32)
                    )
            halves.append(jnp.concatenate(tiles, axis=1))
        total = None
        if project:
            for part in pix:
                total = part if total is None else total + part
            total = fold(total)
        return halves, total

    def dot_all(xs, ys):
        both = sum(jnp.sum(x * y, axis=0, keepdims=True) for x, y in zip(xs, ys))
        return jnp.sum(both, axis=1, keepdims=True)

    right_lhs = split_rows(wgt[...])

    def opening(order):
        def ready(c):
            a, z, copy = chunks[c]
            copy.wait()
            halve_rows(a, z)

        ready(order[0])
        for i, c in enumerate(order):
            h = c // GROUPS
            if i + 1 < len(order):
                ready(order[i + 1])
            to_coef(0, right_lhs, c * gt, c * gt, gt)
            if i == 0:
                pl.semaphore_wait(barrier, waited)
            first = (c % GROUPS) * gt
            send_pieces(0, h, [(j, p) for j, p in every_piece if first < p[1] <= first + gt])

    waited = jnp.where(is_owner, 2 * nh - 1, 2 * nh)

    @pl.when(low)
    def _():
        opening(low_order)

    @pl.when(jnp.logical_not(low))
    def _():
        opening(high_order)

    turn_basis()
    histogram(cnt, lambda here: ivar[here, :])
    own(0)
    sums, seen = consume(0, True)
    scale = 1 / jnp.sqrt(F32(total_pix))
    mean = F32(1 / total_pix)
    residual = [x * scale for x in sums]
    direction = residual
    answer = [jnp.zeros_like(x) for x in residual]
    norm_now = dot_all(residual, residual)

    def first_settle(t, part):
        here = part * scale
        loc[t] = here
        snd[1, t] = here

    settle = first_settle
    for it in range(ITERS):
        last = it + 1 == ITERS
        produce(it + 1, cnt[...] * seen, settle)
        own(it + 1)
        sums, seen = consume(it + 1, not last)
        image = [x * mean + RIDGE * d for x, d in zip(sums, direction)]
        step_len = norm_now / dot_all(direction, image)
        answer = [x + step_len * d for x, d in zip(answer, direction)]
        residual = [x - step_len * y for x, y in zip(residual, image)]
        if not last:
            norm_next = dot_all(residual, residual)
            rate = norm_next / norm_now
            direction = [x + rate * d for x, d in zip(residual, direction)]
            norm_now = norm_next

            def settle(t, part, s=it + 1, step_len=step_len, rate=rate):
                old = snd[s, t]
                here = loc[t] - step_len * (part * mean + RIDGE * old)
                loc[t] = here
                snd[s + 1, t] = here + rate * old

    def ordered(pair):
        return jnp.concatenate(
            [jnp.where(low, pair[0], pair[1]), jnp.where(low, pair[1], pair[0])], axis=1
        )

    out_ref[0] = ordered(answer)[:BANDS, :ncoef]
    out_ref[1] = ordered(residual)[:BANDS, :ncoef]

    first = my_piece * ht // nh
    size = (my_piece + 1) * ht // nh - first
    for n in plan.sizes:
        @pl.when(is_owner & (size == n))
        def _():
            for s in range(STEPS):
                landed(snd.at[s, pl.ds(0, 2 * ht - n), pl.ds(0, BANDS)], send_sems.at[s, 0])
                landed(rsb.at[s, pl.ds(0, ndev - 1), pl.ds(0, n), pl.ds(0, BANDS)], send_sems.at[s, 1])

    @pl.when(jnp.logical_not(is_owner))
    def _():
        for s in range(STEPS):
            landed(snd.at[s, pl.ds(0, 2 * ht), pl.ds(0, BANDS)], send_sems.at[s, 0])


def body(basis, pixel_ids, band_ids, mags, inv_var):
    pixels, ncoef = basis.shape
    objs = pixel_ids.shape[0]
    plan = Plan(lax.axis_size("tile"), lax.axis_size("grp"), ncoef)
    cfg = (pixels, ncoef, objs, plan)
    fold_objs = lambda x: x.reshape(objs // LANES, LANES)
    anyspec = pl.BlockSpec(memory_space=pl.ANY)
    out = jax.ShapeDtypeStruct((2, BANDS, ncoef), F32)
    orow = objs // LANES
    both = pl.pallas_call(
        functools.partial(kernel, cfg),
        out_shape=out,
        in_specs=[anyspec] * 5,
        out_specs=pl.BlockSpec(memory_space=pltpu.VMEM),
        scratch_shapes=[
            pltpu.VMEM((ncoef, pixels), F32),
            pltpu.VMEM((orow, LANES), jnp.int32),
            pltpu.VMEM((orow, LANES), jnp.int32),
            pltpu.VMEM((orow, LANES), F32),
            pltpu.VMEM((orow, LANES), F32),
            pltpu.VMEM((plan.width, pixels), BF16),
            pltpu.VMEM((plan.width, pixels), F8),
            pltpu.VMEM((pixels, plan.width), BF16),
            pltpu.VMEM((pixels, plan.width), F8),
            pltpu.VMEM((8, pixels), F32),
            pltpu.VMEM((8, pixels), F32),
            pltpu.VMEM((STEPS, 2 * plan.ht, 8, LANES), F32),
            pltpu.VMEM((2 * plan.ht, 8, LANES), F32),
            pltpu.VMEM((STEPS, plan.ndev, plan.largest, 8, LANES), F32),
            pltpu.VMEM((STEPS, 2 * plan.ht, 8, LANES), F32),
            pltpu.SemaphoreType.DMA((4 + 2 * GROUPS,)),
            pltpu.SemaphoreType.DMA((STEPS, 2)),
            pltpu.SemaphoreType.DMA((STEPS,)),
            pltpu.SemaphoreType.DMA((STEPS, 2, GROUPS)),
        ],
        compiler_params=pltpu.CompilerParams(collective_id=0, has_side_effects=True),
    )(basis.T, fold_objs(pixel_ids), fold_objs(band_ids), fold_objs(mags), fold_objs(inv_var))
    return both[0], both[1]


def solution(mesh):
    placed = (
        P(("tile", "grp"), None),
        P(("tile", "grp")),
        P(("tile", "grp")),
        P(("tile", "grp")),
        P(("tile", "grp")),
    )
    return jax.shard_map(body, mesh=mesh, in_specs=placed, out_specs=(P(), P()), check_vma=False)
```

```python
import functools

import jax
import jax.numpy as jnp
from jax import lax
from jax.experimental import pallas as pl
from jax.experimental.pallas import tpu as pltpu
from jax.sharding import PartitionSpec as P

BANDS = 5
ITERS = 3
RIDGE = 0.1
STEPS = ITERS + 1
LANES = 128
F32 = jnp.float32
BF16 = jnp.bfloat16
F8 = jnp.float8_e4m3fn
SHIFT = 1024.0
MESH = pl.DeviceIdType.MESH

UNROLL = 64
MIDDLE = 4
SKIP = 2
ODD = 1
SUB = 32
GROUPS = 2


def split_rows(value):
    high = value.astype(BF16).astype(F32)
    both = jnp.concatenate([high, value - high], axis=0)
    return both.astype(BF16), (both * (1 / SHIFT)).astype(BF16)


def fold(value):
    return value[:8] + value[8:]


def tree(terms):
    while len(terms) > 1:
        terms = [
            terms[i] + terms[i + 1] if i + 1 < len(terms) else terms[i]
            for i in range(0, len(terms), 2)
        ]
    return terms[0]


class Plan:
    def __init__(self, tsize, gsize, ncoef):
        self.tsize, self.gsize, self.ndev = tsize, gsize, tsize * gsize
        whole = tsize % MIDDLE == 0
        self.t0, self.tcount = (tsize // MIDDLE, tsize // 2) if whole else (0, tsize)
        self.skip, self.odd = (SKIP, ODD) if gsize % SKIP == 0 else (1, 0)
        self.per_tile = gsize // self.skip
        self.side = self.tcount * self.per_tile // 2
        self.ktiles = -(-ncoef // LANES)
        self.ht = -(-self.ktiles // 2)
        self.ht += -self.ht % GROUPS
        self.gt = self.ht // GROUPS
        self.nh = min(self.side, self.ht)
        self.pieces = [(j * self.ht // self.nh, (j + 1) * self.ht // self.nh) for j in range(self.nh)]
        self.sizes = sorted({b - a for a, b in self.pieces})
        self.largest = max(self.sizes)
        self.width = 2 * self.ht * LANES


def kernel(
    cfg,
    basis_hbm, pid_hbm, bid_hbm, mag_hbm, ivar_hbm,
    out_ref,
    bas, pid, bid, mag, ivar,
    bhi, blo, thi, tlo, cnt, wgt,
    snd, loc, rsb, agb,
    in_sems, send_sems, rs_sems, ag_sems,
):
    pixels, ncoef, objs, plan = cfg
    ht, gt, nh = plan.ht, plan.gt, plan.nh
    ndev, tsize, gsize = plan.ndev, plan.tsize, plan.gsize
    total_pix = pixels * ndev
    hrows = ht * LANES
    grows = gt * LANES

    tile = lax.axis_index("tile")
    grp = lax.axis_index("grp")
    me = tile * gsize + grp
    inside = (tile >= plan.t0) & (tile < plan.t0 + plan.tcount) & (lax.rem(grp, plan.skip) == plan.odd)
    k = (tile - plan.t0) * plan.per_tile + grp // plan.skip
    my_half = k // plan.side
    my_piece = k - my_half * plan.side
    is_owner = inside & (my_piece < nh)
    low = tile < tsize // 2
    near = jnp.where(low, 0, 1)
    far = 1 - near
    same = lax.rem(tile, GROUPS)
    other = 1 - same

    def at(t, g):
        return {"tile": t, "grp": g}

    def owner_place(h, j):
        o = h * plan.side + j
        return plan.t0 + o // plan.per_tile, lax.rem(o, plan.per_tile) * plan.skip + plan.odd

    barrier = pltpu.get_barrier_semaphore()

    def steps(n, shift):
        return min(shift, n - shift)

    def reach(move):
        a, b = move
        outer, inner = (a // 2, a % 2) if tsize % 2 == 0 else (a, 0)
        return -(
            steps(max(tsize // 2, 1), outer) + inner
            + steps(max(gsize // 2, 1), (b + 1) // 2 % max(gsize // 2, 1)) + (b % 2) * 0.95
        )

    def toward(a, b):
        g = lax.rem(grp + b, gsize)
        if tsize % 2:
            return lax.rem(tile + a, tsize), g
        outer = lax.rem(tile // 2 + a // 2, tsize // 2)
        return outer * 2 + lax.rem(tile + a % 2, 2), g

    def everyone(send):
        moves = sorted(((a, b) for a in range(tsize) for b in range(gsize) if a or b), key=reach)
        if ndev - 1 <= UNROLL:
            for a, b in moves:
                send(*toward(a, b))
        else:
            def some(i, _):
                a = lax.rem(i // gsize + tsize // 2, tsize)
                b = lax.rem(i, gsize)

                @pl.when(i != (tsize - tsize // 2) * gsize)
                def _():
                    send(lax.rem(tile + a, tsize), lax.rem(grp + b, gsize))
                return 0

            lax.fori_loop(0, ndev, some, 0)

    @pl.when(is_owner)
    def _():
        everyone(
            lambda t, g: pl.semaphore_signal(barrier, inc=1, device_id=at(t, g), device_id_type=MESH)
        )

    small = []
    for i, (src, dst) in enumerate(((pid_hbm, pid), (bid_hbm, bid), (mag_hbm, mag), (ivar_hbm, ivar))):
        c = pltpu.make_async_copy(src, dst, in_sems.at[i])
        c.start()
        small.append(c)

    chunks = []
    for c in range(2 * GROUPS):
        a, z = c * grows, min((c + 1) * grows, ncoef)
        rows = pl.ds(a, z - a)
        chunks.append((a, z, pltpu.make_async_copy(basis_hbm.at[rows, :], bas.at[rows, :], in_sems.at[4 + c])))
    low_order = list(range(GROUPS, 2 * GROUPS)) + list(range(GROUPS))
    high_order = list(range(2 * GROUPS))

    @pl.when(low)
    def _():
        for c in low_order:
            chunks[c][2].start()

    @pl.when(jnp.logical_not(low))
    def _():
        for c in high_order:
            chunks[c][2].start()

    cnt[...] = jnp.zeros_like(cnt)
    wgt[...] = jnp.zeros_like(wgt)
    agb[...] = jnp.zeros_like(agb)

    for c in small:
        c.wait()
    blocks = pixels // LANES
    keys = -(-BANDS * blocks // 8) * 8
    orow = objs // LANES
    step_rows = 8 if orow % 8 == 0 else 1

    def histogram(dst, value_of):
        def hist_step(i, acc):
            lhs_parts, rhs_parts = [], []
            for r in range(step_rows):
                here = pl.ds(i * step_rows + r, 1)
                pix = pid[here, :]
                key = bid[here, :] * blocks + pix // LANES
                lane = lax.rem(pix, LANES)
                hot = lax.broadcasted_iota(jnp.int32, (LANES, LANES), 0) == lane
                rhs_parts.append(jnp.where(hot, F32(1), F32(0)).astype(F8))
                sel = lax.broadcasted_iota(jnp.int32, (keys, LANES), 0) == key
                value = value_of(here)
                high = value.astype(BF16).astype(F32)
                lhs_parts.append(
                    jnp.concatenate(
                        [jnp.where(sel, x, F32(0)) for x in (high, value - high)], axis=0
                    ).astype(BF16)
                )
            lhs = jnp.concatenate(lhs_parts, axis=1)
            rhs = jnp.concatenate(rhs_parts, axis=1)
            return acc + lax.dot_general(
                lhs, rhs, (((1,), (1,)), ((), ())), preferred_element_type=F32
            )

        acc = lax.fori_loop(
            0, orow // step_rows, hist_step, jnp.zeros((2 * keys, LANES), F32), unroll=4
        )
        both = acc[:keys] + acc[keys:]
        for b in range(BANDS):
            for j in range(blocks):
                r = b * blocks + j
                dst[b : b + 1, j * LANES : (j + 1) * LANES] = both[r : r + 1]

    histogram(wgt, lambda here: ivar[here, :] * mag[here, :])

    def halve(rows, x):
        h = x.astype(BF16)
        bhi[rows, :] = h
        blo[rows, :] = ((x - h.astype(F32)) * SHIFT).astype(F8)

    def halve_rows(a, z):
        full = (z - a) // SUB

        for i in range(a, a + full * SUB, SUB):
            halve(slice(i, i + SUB), bas[i : i + SUB, :])

        done = a + full * SUB
        if done < z:
            pad = jnp.zeros((SUB - (z - done), pixels), F32)
            halve(slice(done, done + SUB), jnp.concatenate([bas[done:z, :], pad], axis=0))

    for z in range(-(-ncoef // SUB) * SUB, plan.width, SUB):
        halve(slice(z, z + SUB), jnp.zeros((SUB, pixels), F32))

    def to_coef(s, lhs, base, first, count):
        dims = (((1,), (1,)), ((), ()))
        for a in range(0, count, 2):
            n = min(2, count - a)
            start = (first + a) * LANES
            if not isinstance(start, int):
                start = pl.multiple_of(start, LANES)
            rows = pl.ds(start, n * LANES)
            part = fold(
                lax.dot_general(lhs[0], bhi[rows, :], dims, preferred_element_type=F32)
                + lax.dot_general(lhs[1], blo[rows, :], dims, preferred_element_type=F32)
            )
            for i in range(n):
                snd[s, base + a + i] = part[:, i * LANES : (i + 1) * LANES]

    def send_group(s, h, group):
        across = grp // plan.skip
        todo = list(enumerate(plan.pieces[: nh // GROUPS]))
        for turn in (0, 1) if len(todo) == 2 else (None,):
            for j, (a, z) in todo:
                t, g = owner_place(h, group * (nh // GROUPS) + j)
                other_device = jnp.logical_not((t == tile) & (g == grp))
                if turn is not None:
                    other_device = other_device & ((across != j) if turn == 0 else (across == j))

                @pl.when(other_device)
                def _():
                    pltpu.make_async_remote_copy(
                        src_ref=snd.at[s, pl.ds(h * ht + group * gt + a, z - a), pl.ds(0, BANDS)],
                        dst_ref=rsb.at[s, me, pl.ds(0, z - a), pl.ds(0, BANDS)],
                        send_sem=send_sems.at[s, 0], recv_sem=rs_sems.at[s],
                        device_id=at(t, g), device_id_type=MESH,
                    ).start()

    def landed(part, sem):
        pltpu.make_async_copy(part, part, sem).wait()

    def turn_basis():
        @pl.loop(0, 2 * ht)
        def _(i):
            rows = pl.ds(pl.multiple_of(i * LANES, LANES), LANES)
            for c in range(0, pixels, LANES):
                thi[c : c + LANES, rows] = bhi[rows, c : c + LANES].T
                tlo[c : c + LANES, rows] = blo[rows, c : c + LANES].T

    def produce(s, scaled, settle):
        lhs = split_rows(scaled)
        for h, g in ((far, other), (far, same), (near, other), (near, same)):
            base = h * ht + g * gt
            for a in range(0, gt, 2):
                n = min(2, gt - a)
                cols = pl.ds(pl.multiple_of((base + a) * LANES, LANES), n * LANES)
                part = fold(
                    jnp.dot(lhs[0], thi[:, cols], preferred_element_type=F32)
                    + jnp.dot(lhs[1], tlo[:, cols], preferred_element_type=F32)
                )
                for i in range(n):
                    settle(base + a + i, part[:, i * LANES : (i + 1) * LANES])
            send_group(s, h, g)

    def own(s):
        for n in plan.sizes:
            first = my_piece * ht // nh
            size = (my_piece + 1) * ht // nh - first

            @pl.when(is_owner & (size == n))
            def _():
                mine = pl.ds(my_half * ht + first, n)
                rsb[s, me, :n] = snd[s, mine]
                landed(rsb.at[s, pl.ds(0, ndev - 1), pl.ds(0, n), pl.ds(0, BANDS)], rs_sems.at[s])
                for i in range(n):
                    agb[s, my_half * ht + first + i, :BANDS] = tree(
                        [rsb[s, d, i, :BANDS] for d in range(ndev)]
                    )
                spread = agb.at[s, mine, pl.ds(0, BANDS)]
                group = first // gt

                def forward(t, g):
                    pltpu.make_async_remote_copy(
                        src_ref=spread, dst_ref=spread,
                        send_sem=send_sems.at[s, 1], recv_sem=ag_sems.at[s, my_half, group],
                        device_id=at(t, g), device_id_type=MESH,
                    ).start()

                everyone(forward)

    def group_wait(s, h, g):
        def part(m):
            return agb.at[s, pl.ds(0, m), pl.ds(0, BANDS)]

        sem = ag_sems.at[s, h, g]
        first = my_piece * ht // nh
        size = (my_piece + 1) * ht // nh - first
        holds = is_owner & (my_half == h) & (first // gt == g)

        @pl.when(jnp.logical_not(holds))
        def _():
            landed(part(gt), sem)

        for n in plan.sizes:
            if n < gt:
                @pl.when(holds & (size == n))
                def _():
                    landed(part(gt - n), sem)

    def consume(s, project):
        quarters, pix = [], []
        for h, g in ((near, same), (near, other), (far, same), (far, other)):
            group_wait(s, h, g)
            here = jnp.concatenate([agb[s, h * ht + g * gt + i] for i in range(gt)], axis=1)
            quarters.append(here)
            if project:
                lhs = split_rows(here)
                rows = pl.ds(pl.multiple_of((h * GROUPS + g) * grows, LANES), grows)
                pix.append(
                    jnp.dot(lhs[0], bhi[rows, :], preferred_element_type=F32)
                    + jnp.dot(lhs[1], blo[rows, :], preferred_element_type=F32)
                )
        total = None
        if project:
            for part in pix:
                total = part if total is None else total + part
            total = fold(total)
        return quarters, total

    def dot_all(xs, ys):
        both = sum(jnp.sum(x * y, axis=0, keepdims=True) for x, y in zip(xs, ys))
        return jnp.sum(both, axis=1, keepdims=True)

    right_lhs = split_rows(wgt[...])

    def opening(order):
        def ready(c):
            a, z, copy = chunks[c]
            copy.wait()
            halve_rows(a, z)

        ready(order[0])
        for i, c in enumerate(order):
            h = c // GROUPS
            if i + 1 < len(order):
                ready(order[i + 1])
            to_coef(0, right_lhs, c * gt, c * gt, gt)
            if i == 0:
                pl.semaphore_wait(barrier, waited)
            send_group(0, h, c % GROUPS)

    waited = jnp.where(is_owner, 2 * nh - 1, 2 * nh)

    @pl.when(low)
    def _():
        opening(low_order)

    @pl.when(jnp.logical_not(low))
    def _():
        opening(high_order)

    turn_basis()
    histogram(cnt, lambda here: ivar[here, :])
    own(0)
    sums, seen = consume(0, True)
    scale = 1 / jnp.sqrt(F32(total_pix))
    mean = F32(1 / total_pix)
    residual = [x * scale for x in sums]
    direction = residual
    answer = [jnp.zeros_like(x) for x in residual]
    norm_now = dot_all(residual, residual)

    def first_settle(t, part):
        here = part * scale
        loc[t] = here
        snd[1, t] = here

    settle = first_settle
    for it in range(ITERS):
        last = it + 1 == ITERS
        produce(it + 1, cnt[...] * seen, settle)
        own(it + 1)
        sums, seen = consume(it + 1, not last)
        image = [x * mean + RIDGE * d for x, d in zip(sums, direction)]
        step_len = norm_now / dot_all(direction, image)
        answer = [x + step_len * d for x, d in zip(answer, direction)]
        residual = [x - step_len * y for x, y in zip(residual, image)]
        if not last:
            norm_next = dot_all(residual, residual)
            rate = norm_next / norm_now
            direction = [x + rate * d for x, d in zip(residual, direction)]
            norm_now = norm_next

            def settle(t, part, s=it + 1, step_len=step_len, rate=rate):
                old = snd[s, t]
                here = loc[t] - step_len * (part * mean + RIDGE * old)
                loc[t] = here
                snd[s + 1, t] = here + rate * old

    def swap(flag, x, y):
        return jnp.where(flag, x, y), jnp.where(flag, y, x)

    def ordered(quarters):
        first = swap(same == 0, *quarters[:2])
        second = swap(same == 0, *quarters[2:])
        pairs = [swap(low, x, y) for x, y in zip(first, second)]
        return jnp.concatenate([pairs[0][0], pairs[1][0], pairs[0][1], pairs[1][1]], axis=1)

    out_ref[0] = ordered(answer)[:BANDS, :ncoef]
    out_ref[1] = ordered(residual)[:BANDS, :ncoef]

    first = my_piece * ht // nh
    size = (my_piece + 1) * ht // nh - first
    for n in plan.sizes:
        @pl.when(is_owner & (size == n))
        def _():
            for s in range(STEPS):
                landed(snd.at[s, pl.ds(0, 2 * ht - n), pl.ds(0, BANDS)], send_sems.at[s, 0])
                landed(rsb.at[s, pl.ds(0, ndev - 1), pl.ds(0, n), pl.ds(0, BANDS)], send_sems.at[s, 1])

    @pl.when(jnp.logical_not(is_owner))
    def _():
        for s in range(STEPS):
            landed(snd.at[s, pl.ds(0, 2 * ht), pl.ds(0, BANDS)], send_sems.at[s, 0])


def body(basis, pixel_ids, band_ids, mags, inv_var):
    pixels, ncoef = basis.shape
    objs = pixel_ids.shape[0]
    plan = Plan(lax.axis_size("tile"), lax.axis_size("grp"), ncoef)
    cfg = (pixels, ncoef, objs, plan)
    fold_objs = lambda x: x.reshape(objs // LANES, LANES)
    anyspec = pl.BlockSpec(memory_space=pl.ANY)
    out = jax.ShapeDtypeStruct((2, BANDS, ncoef), F32)
    orow = objs // LANES
    both = pl.pallas_call(
        functools.partial(kernel, cfg),
        out_shape=out,
        in_specs=[anyspec] * 5,
        out_specs=pl.BlockSpec(memory_space=pltpu.VMEM),
        scratch_shapes=[
            pltpu.VMEM((ncoef, pixels), F32),
            pltpu.VMEM((orow, LANES), jnp.int32),
            pltpu.VMEM((orow, LANES), jnp.int32),
            pltpu.VMEM((orow, LANES), F32),
            pltpu.VMEM((orow, LANES), F32),
            pltpu.VMEM((plan.width, pixels), BF16),
            pltpu.VMEM((plan.width, pixels), F8),
            pltpu.VMEM((pixels, plan.width), BF16),
            pltpu.VMEM((pixels, plan.width), F8),
            pltpu.VMEM((8, pixels), F32),
            pltpu.VMEM((8, pixels), F32),
            pltpu.VMEM((STEPS, 2 * plan.ht, 8, LANES), F32),
            pltpu.VMEM((2 * plan.ht, 8, LANES), F32),
            pltpu.VMEM((STEPS, plan.ndev, plan.largest, 8, LANES), F32),
            pltpu.VMEM((STEPS, 2 * plan.ht, 8, LANES), F32),
            pltpu.SemaphoreType.DMA((4 + 2 * GROUPS,)),
            pltpu.SemaphoreType.DMA((STEPS, 2)),
            pltpu.SemaphoreType.DMA((STEPS,)),
            pltpu.SemaphoreType.DMA((STEPS, 2, GROUPS)),
        ],
        compiler_params=pltpu.CompilerParams(collective_id=0, has_side_effects=True),
    )(basis.T, fold_objs(pixel_ids), fold_objs(band_ids), fold_objs(mags), fold_objs(inv_var))
    return both[0], both[1]


def solution(mesh):
    placed = (
        P(("tile", "grp"), None),
        P(("tile", "grp")),
        P(("tile", "grp")),
        P(("tile", "grp")),
        P(("tile", "grp")),
    )
    return jax.shard_map(body, mesh=mesh, in_specs=placed, out_specs=(P(), P()), check_vma=False)
```

```python
import functools

import jax
import jax.numpy as jnp
from jax import lax
from jax.experimental import pallas as pl
from jax.experimental.pallas import tpu as pltpu
from jax.sharding import PartitionSpec as P

BANDS = 5
ITERS = 3
RIDGE = 0.1
STEPS = ITERS + 1
LANES = 128
F32 = jnp.float32
BF16 = jnp.bfloat16
F8 = jnp.float8_e4m3fn
SHIFT = 1024.0
MESH = pl.DeviceIdType.MESH

UNROLL = 64
MIDDLE = 4
SKIP = 2
ODD = 1
SUB = 32
GROUPS = 2


def split_rows(value):
    high = value.astype(BF16).astype(F32)
    both = jnp.concatenate([high, value - high], axis=0)
    return both.astype(BF16), (both * (1 / SHIFT)).astype(BF16)


def fold(value):
    return value[:8] + value[8:]


def tree(terms):
    while len(terms) > 1:
        terms = [
            terms[i] + terms[i + 1] if i + 1 < len(terms) else terms[i]
            for i in range(0, len(terms), 2)
        ]
    return terms[0]


class Plan:
    def __init__(self, tsize, gsize, ncoef):
        self.tsize, self.gsize, self.ndev = tsize, gsize, tsize * gsize
        whole = tsize % MIDDLE == 0
        self.t0, self.tcount = (tsize // MIDDLE, tsize // 2) if whole else (0, tsize)
        self.skip, self.odd = (SKIP, ODD) if gsize % SKIP == 0 else (1, 0)
        self.per_tile = gsize // self.skip
        self.side = self.tcount * self.per_tile // 2
        self.ktiles = -(-ncoef // LANES)
        self.ht = -(-self.ktiles // 2)
        self.ht += -self.ht % GROUPS
        self.gt = self.ht // GROUPS
        self.nh = min(self.side, self.ht)
        self.pieces = [(j * self.ht // self.nh, (j + 1) * self.ht // self.nh) for j in range(self.nh)]
        self.sizes = sorted({b - a for a, b in self.pieces})
        self.largest = max(self.sizes)
        self.width = 2 * self.ht * LANES


def kernel(
    cfg,
    basis_hbm, pid_hbm, bid_hbm, mag_hbm, ivar_hbm,
    out_ref,
    bas, pid, bid, mag, ivar,
    bhi, blo, thi, tlo, cnt, wgt,
    snd, loc, rsb, agb,
    in_sems, send_sems, rs_sems, ag_sems,
):
    pixels, ncoef, objs, plan = cfg
    ht, gt, nh = plan.ht, plan.gt, plan.nh
    ndev, tsize, gsize = plan.ndev, plan.tsize, plan.gsize
    total_pix = pixels * ndev
    hrows = ht * LANES
    grows = gt * LANES

    tile = lax.axis_index("tile")
    grp = lax.axis_index("grp")
    me = tile * gsize + grp
    inside = (tile >= plan.t0) & (tile < plan.t0 + plan.tcount) & (lax.rem(grp, plan.skip) == plan.odd)
    k = (tile - plan.t0) * plan.per_tile + grp // plan.skip
    my_half = k // plan.side
    my_piece = k - my_half * plan.side
    is_owner = inside & (my_piece < nh)
    low = tile < tsize // 2
    near = jnp.where(low, 0, 1)
    far = 1 - near
    same = lax.rem(tile, GROUPS)
    other = 1 - same

    def at(t, g):
        return {"tile": t, "grp": g}

    def owner_place(h, j):
        o = h * plan.side + j
        return plan.t0 + o // plan.per_tile, lax.rem(o, plan.per_tile) * plan.skip + plan.odd

    barrier = pltpu.get_barrier_semaphore()

    def steps(n, shift):
        return min(shift, n - shift)

    def reach(move):
        a, b = move
        outer, inner = (a // 2, a % 2) if tsize % 2 == 0 else (a, 0)
        return -(
            steps(max(tsize // 2, 1), outer) + inner
            + steps(max(gsize // 2, 1), (b + 1) // 2 % max(gsize // 2, 1)) * 1.5 + (b % 2) * 0.95
        )

    def toward(a, b):
        g = lax.rem(grp + b, gsize)
        if tsize % 2:
            return lax.rem(tile + a, tsize), g
        outer = lax.rem(tile // 2 + a // 2, tsize // 2)
        return outer * 2 + lax.rem(tile + a % 2, 2), g

    def everyone(send):
        moves = sorted(((a, b) for a in range(tsize) for b in range(gsize) if a or b), key=reach)
        if ndev - 1 <= UNROLL:
            for a, b in moves:
                send(*toward(a, b))
        else:
            def some(i, _):
                a = lax.rem(i // gsize + tsize // 2, tsize)
                b = lax.rem(i, gsize)

                @pl.when(i != (tsize - tsize // 2) * gsize)
                def _():
                    send(lax.rem(tile + a, tsize), lax.rem(grp + b, gsize))
                return 0

            lax.fori_loop(0, ndev, some, 0)

    @pl.when(is_owner)
    def _():
        everyone(
            lambda t, g: pl.semaphore_signal(barrier, inc=1, device_id=at(t, g), device_id_type=MESH)
        )

    small = []
    for i, (src, dst) in enumerate(((pid_hbm, pid), (bid_hbm, bid), (mag_hbm, mag), (ivar_hbm, ivar))):
        c = pltpu.make_async_copy(src, dst, in_sems.at[i])
        c.start()
        small.append(c)

    chunks = []
    for c in range(2 * GROUPS):
        a, z = c * grows, min((c + 1) * grows, ncoef)
        rows = pl.ds(a, z - a)
        chunks.append((a, z, pltpu.make_async_copy(basis_hbm.at[rows, :], bas.at[rows, :], in_sems.at[4 + c])))
    low_order = list(range(GROUPS, 2 * GROUPS)) + list(range(GROUPS))
    high_order = list(range(2 * GROUPS))

    @pl.when(low)
    def _():
        for c in low_order:
            chunks[c][2].start()

    @pl.when(jnp.logical_not(low))
    def _():
        for c in high_order:
            chunks[c][2].start()

    cnt[...] = jnp.zeros_like(cnt)
    wgt[...] = jnp.zeros_like(wgt)
    agb[...] = jnp.zeros_like(agb)

    for c in small:
        c.wait()
    blocks = pixels // LANES
    keys = -(-BANDS * blocks // 8) * 8
    orow = objs // LANES
    step_rows = 8 if orow % 8 == 0 else 1

    def histogram(dst, value_of):
        def hist_step(i, acc):
            lhs_parts, rhs_parts = [], []
            for r in range(step_rows):
                here = pl.ds(i * step_rows + r, 1)
                pix = pid[here, :]
                key = bid[here, :] * blocks + pix // LANES
                lane = lax.rem(pix, LANES)
                hot = lax.broadcasted_iota(jnp.int32, (LANES, LANES), 0) == lane
                rhs_parts.append(jnp.where(hot, F32(1), F32(0)).astype(F8))
                sel = lax.broadcasted_iota(jnp.int32, (keys, LANES), 0) == key
                value = value_of(here)
                high = value.astype(BF16).astype(F32)
                lhs_parts.append(
                    jnp.concatenate(
                        [jnp.where(sel, x, F32(0)) for x in (high, value - high)], axis=0
                    ).astype(BF16)
                )
            lhs = jnp.concatenate(lhs_parts, axis=1)
            rhs = jnp.concatenate(rhs_parts, axis=1)
            return acc + lax.dot_general(
                lhs, rhs, (((1,), (1,)), ((), ())), preferred_element_type=F32
            )

        acc = lax.fori_loop(
            0, orow // step_rows, hist_step, jnp.zeros((2 * keys, LANES), F32), unroll=4
        )
        both = acc[:keys] + acc[keys:]
        for b in range(BANDS):
            for j in range(blocks):
                r = b * blocks + j
                dst[b : b + 1, j * LANES : (j + 1) * LANES] = both[r : r + 1]

    histogram(wgt, lambda here: ivar[here, :] * mag[here, :])

    def halve(rows, x):
        h = x.astype(BF16)
        bhi[rows, :] = h
        blo[rows, :] = ((x - h.astype(F32)) * SHIFT).astype(F8)

    def halve_rows(a, z):
        full = (z - a) // SUB

        for i in range(a, a + full * SUB, SUB):
            halve(slice(i, i + SUB), bas[i : i + SUB, :])

        done = a + full * SUB
        if done < z:
            pad = jnp.zeros((SUB - (z - done), pixels), F32)
            halve(slice(done, done + SUB), jnp.concatenate([bas[done:z, :], pad], axis=0))

    for z in range(-(-ncoef // SUB) * SUB, plan.width, SUB):
        halve(slice(z, z + SUB), jnp.zeros((SUB, pixels), F32))

    def to_coef(s, lhs, base, first, count):
        dims = (((1,), (1,)), ((), ()))
        for a in range(0, count, 2):
            n = min(2, count - a)
            start = (first + a) * LANES
            if not isinstance(start, int):
                start = pl.multiple_of(start, LANES)
            rows = pl.ds(start, n * LANES)
            part = fold(
                lax.dot_general(lhs[0], bhi[rows, :], dims, preferred_element_type=F32)
                + lax.dot_general(lhs[1], blo[rows, :], dims, preferred_element_type=F32)
            )
            for i in range(n):
                snd[s, base + a + i] = part[:, i * LANES : (i + 1) * LANES]

    def send_group(s, h, group):
        across = grp // plan.skip
        todo = list(enumerate(plan.pieces[: nh // GROUPS]))
        for turn in (0, 1) if len(todo) == 2 else (None,):
            for j, (a, z) in todo:
                t, g = owner_place(h, group * (nh // GROUPS) + j)
                other_device = jnp.logical_not((t == tile) & (g == grp))
                if turn is not None:
                    other_device = other_device & ((across != j) if turn == 0 else (across == j))

                @pl.when(other_device)
                def _():
                    pltpu.make_async_remote_copy(
                        src_ref=snd.at[s, pl.ds(h * ht + group * gt + a, z - a), pl.ds(0, BANDS)],
                        dst_ref=rsb.at[s, me, pl.ds(0, z - a), pl.ds(0, BANDS)],
                        send_sem=send_sems.at[s, 0], recv_sem=rs_sems.at[s],
                        device_id=at(t, g), device_id_type=MESH,
                    ).start()

    def landed(part, sem):
        pltpu.make_async_copy(part, part, sem).wait()

    def turn_basis():
        @pl.loop(0, 2 * ht)
        def _(i):
            rows = pl.ds(pl.multiple_of(i * LANES, LANES), LANES)
            for c in range(0, pixels, LANES):
                thi[c : c + LANES, rows] = bhi[rows, c : c + LANES].T
                tlo[c : c + LANES, rows] = blo[rows, c : c + LANES].T

    def produce(s, scaled, settle):
        lhs = split_rows(scaled)
        for h, g in ((far, other), (far, same), (near, other), (near, same)):
            base = h * ht + g * gt
            for a in range(0, gt, 2):
                n = min(2, gt - a)
                cols = pl.ds(pl.multiple_of((base + a) * LANES, LANES), n * LANES)
                part = fold(
                    jnp.dot(lhs[0], thi[:, cols], preferred_element_type=F32)
                    + jnp.dot(lhs[1], tlo[:, cols], preferred_element_type=F32)
                )
                for i in range(n):
                    settle(base + a + i, part[:, i * LANES : (i + 1) * LANES])
            send_group(s, h, g)

    def own(s):
        for n in plan.sizes:
            first = my_piece * ht // nh
            size = (my_piece + 1) * ht // nh - first

            @pl.when(is_owner & (size == n))
            def _():
                mine = pl.ds(my_half * ht + first, n)
                rsb[s, me, :n] = snd[s, mine]
                landed(rsb.at[s, pl.ds(0, ndev - 1), pl.ds(0, n), pl.ds(0, BANDS)], rs_sems.at[s])
                for i in range(n):
                    agb[s, my_half * ht + first + i, :BANDS] = tree(
                        [rsb[s, d, i, :BANDS] for d in range(ndev)]
                    )
                spread = agb.at[s, mine, pl.ds(0, BANDS)]
                group = first // gt

                def forward(t, g):
                    pltpu.make_async_remote_copy(
                        src_ref=spread, dst_ref=spread,
                        send_sem=send_sems.at[s, 1], recv_sem=ag_sems.at[s, my_half, group],
                        device_id=at(t, g), device_id_type=MESH,
                    ).start()

                everyone(forward)

    def group_wait(s, h, g):
        def part(m):
            return agb.at[s, pl.ds(0, m), pl.ds(0, BANDS)]

        sem = ag_sems.at[s, h, g]
        first = my_piece * ht // nh
        size = (my_piece + 1) * ht // nh - first
        holds = is_owner & (my_half == h) & (first // gt == g)

        @pl.when(jnp.logical_not(holds))
        def _():
            landed(part(gt), sem)

        for n in plan.sizes:
            if n < gt:
                @pl.when(holds & (size == n))
                def _():
                    landed(part(gt - n), sem)

    def consume(s, project):
        quarters, pix = [], []
        for h, g in ((near, same), (near, other), (far, same), (far, other)):
            group_wait(s, h, g)
            here = jnp.concatenate([agb[s, h * ht + g * gt + i] for i in range(gt)], axis=1)
            quarters.append(here)
            if project:
                lhs = split_rows(here)
                rows = pl.ds(pl.multiple_of((h * GROUPS + g) * grows, LANES), grows)
                pix.append(
                    jnp.dot(lhs[0], bhi[rows, :], preferred_element_type=F32)
                    + jnp.dot(lhs[1], blo[rows, :], preferred_element_type=F32)
                )
        total = None
        if project:
            for part in pix:
                total = part if total is None else total + part
            total = fold(total)
        return quarters, total

    def dot_all(xs, ys):
        both = sum(jnp.sum(x * y, axis=0, keepdims=True) for x, y in zip(xs, ys))
        return jnp.sum(both, axis=1, keepdims=True)

    right_lhs = split_rows(wgt[...])

    def opening(order):
        def ready(c):
            a, z, copy = chunks[c]
            copy.wait()
            halve_rows(a, z)

        ready(order[0])
        for i, c in enumerate(order):
            h = c // GROUPS
            if i + 1 < len(order):
                ready(order[i + 1])
            to_coef(0, right_lhs, c * gt, c * gt, gt)
            if i == 0:
                pl.semaphore_wait(barrier, waited)
            send_group(0, h, c % GROUPS)

    waited = jnp.where(is_owner, 2 * nh - 1, 2 * nh)

    @pl.when(low)
    def _():
        opening(low_order)

    @pl.when(jnp.logical_not(low))
    def _():
        opening(high_order)

    turn_basis()
    own(0)
    histogram(cnt, lambda here: ivar[here, :])
    sums, seen = consume(0, True)
    scale = 1 / jnp.sqrt(F32(total_pix))
    mean = F32(1 / total_pix)
    residual = [x * scale for x in sums]
    direction = residual
    answer = [jnp.zeros_like(x) for x in residual]
    norm_now = dot_all(residual, residual)

    def first_settle(t, part):
        here = part * scale
        loc[t] = here
        snd[1, t] = here

    settle = first_settle
    for it in range(ITERS):
        last = it + 1 == ITERS
        produce(it + 1, cnt[...] * seen, settle)
        own(it + 1)
        sums, seen = consume(it + 1, not last)
        image = [x * mean + RIDGE * d for x, d in zip(sums, direction)]
        step_len = norm_now / dot_all(direction, image)
        answer = [x + step_len * d for x, d in zip(answer, direction)]
        residual = [x - step_len * y for x, y in zip(residual, image)]
        if not last:
            norm_next = dot_all(residual, residual)
            rate = norm_next / norm_now
            direction = [x + rate * d for x, d in zip(residual, direction)]
            norm_now = norm_next

            def settle(t, part, s=it + 1, step_len=step_len, rate=rate):
                old = snd[s, t]
                here = loc[t] - step_len * (part * mean + RIDGE * old)
                loc[t] = here
                snd[s + 1, t] = here + rate * old

    def swap(flag, x, y):
        return jnp.where(flag, x, y), jnp.where(flag, y, x)

    def ordered(quarters):
        first = swap(same == 0, *quarters[:2])
        second = swap(same == 0, *quarters[2:])
        pairs = [swap(low, x, y) for x, y in zip(first, second)]
        return jnp.concatenate([pairs[0][0], pairs[1][0], pairs[0][1], pairs[1][1]], axis=1)

    out_ref[0] = ordered(answer)[:, : plan.ktiles * LANES]
    out_ref[1] = ordered(residual)[:, : plan.ktiles * LANES]

    first = my_piece * ht // nh
    size = (my_piece + 1) * ht // nh - first
    for n in plan.sizes:
        @pl.when(is_owner & (size == n))
        def _():
            for s in range(STEPS):
                landed(snd.at[s, pl.ds(0, 2 * ht - n), pl.ds(0, BANDS)], send_sems.at[s, 0])
                landed(rsb.at[s, pl.ds(0, ndev - 1), pl.ds(0, n), pl.ds(0, BANDS)], send_sems.at[s, 1])

    @pl.when(jnp.logical_not(is_owner))
    def _():
        for s in range(STEPS):
            landed(snd.at[s, pl.ds(0, 2 * ht), pl.ds(0, BANDS)], send_sems.at[s, 0])


def body(basis, pixel_ids, band_ids, mags, inv_var):
    pixels, ncoef = basis.shape
    objs = pixel_ids.shape[0]
    plan = Plan(lax.axis_size("tile"), lax.axis_size("grp"), ncoef)
    cfg = (pixels, ncoef, objs, plan)
    fold_objs = lambda x: x.reshape(objs // LANES, LANES)
    anyspec = pl.BlockSpec(memory_space=pl.ANY)
    out = jax.ShapeDtypeStruct((2, 8, plan.ktiles * LANES), F32)
    orow = objs // LANES
    both = pl.pallas_call(
        functools.partial(kernel, cfg),
        out_shape=out,
        in_specs=[anyspec] * 5,
        out_specs=pl.BlockSpec(memory_space=pltpu.VMEM),
        scratch_shapes=[
            pltpu.VMEM((ncoef, pixels), F32),
            pltpu.VMEM((orow, LANES), jnp.int32),
            pltpu.VMEM((orow, LANES), jnp.int32),
            pltpu.VMEM((orow, LANES), F32),
            pltpu.VMEM((orow, LANES), F32),
            pltpu.VMEM((plan.width, pixels), BF16),
            pltpu.VMEM((plan.width, pixels), F8),
            pltpu.VMEM((pixels, plan.width), BF16),
            pltpu.VMEM((pixels, plan.width), F8),
            pltpu.VMEM((8, pixels), F32),
            pltpu.VMEM((8, pixels), F32),
            pltpu.VMEM((STEPS, 2 * plan.ht, 8, LANES), F32),
            pltpu.VMEM((2 * plan.ht, 8, LANES), F32),
            pltpu.VMEM((STEPS, plan.ndev, plan.largest, 8, LANES), F32),
            pltpu.VMEM((STEPS, 2 * plan.ht, 8, LANES), F32),
            pltpu.SemaphoreType.DMA((4 + 2 * GROUPS,)),
            pltpu.SemaphoreType.DMA((STEPS, 2)),
            pltpu.SemaphoreType.DMA((STEPS,)),
            pltpu.SemaphoreType.DMA((STEPS, 2, GROUPS)),
        ],
        compiler_params=pltpu.CompilerParams(collective_id=0, has_side_effects=True),
    )(basis.T, fold_objs(pixel_ids), fold_objs(band_ids), fold_objs(mags), fold_objs(inv_var))
    return both[0, :BANDS, :ncoef], both[1, :BANDS, :ncoef]


def solution(mesh):
    placed = (
        P(("tile", "grp"), None),
        P(("tile", "grp")),
        P(("tile", "grp")),
        P(("tile", "grp")),
        P(("tile", "grp")),
    )
    return jax.shard_map(body, mesh=mesh, in_specs=placed, out_specs=(P(), P()), check_vma=False)
```

```python
import functools

import jax
import jax.numpy as jnp
from jax import lax
from jax.experimental import pallas as pl
from jax.experimental.pallas import tpu as pltpu
from jax.sharding import PartitionSpec as P

BANDS = 5
ITERS = 3
RIDGE = 0.1
STEPS = ITERS + 1
LANES = 128
F32 = jnp.float32
BF16 = jnp.bfloat16
F8 = jnp.float8_e4m3fn
SHIFT = 1024.0
MESH = pl.DeviceIdType.MESH

UNROLL = 64
MIDDLE = 4
SKIP = 2
ODD = 1
SUB = 32
GROUPS = 2


def split_rows(value):
    high = value.astype(BF16).astype(F32)
    both = jnp.concatenate([high, value - high], axis=0)
    return both.astype(BF16), (both * (1 / SHIFT)).astype(BF16)


def fold(value):
    return value[:8] + value[8:]


def tree(terms):
    while len(terms) > 1:
        terms = [
            terms[i] + terms[i + 1] if i + 1 < len(terms) else terms[i]
            for i in range(0, len(terms), 2)
        ]
    return terms[0]


class Plan:
    def __init__(self, tsize, gsize, ncoef):
        self.tsize, self.gsize, self.ndev = tsize, gsize, tsize * gsize
        whole = tsize % MIDDLE == 0
        self.t0, self.tcount = (tsize // MIDDLE, tsize // 2) if whole else (0, tsize)
        self.skip, self.odd = (SKIP, ODD) if gsize % SKIP == 0 else (1, 0)
        self.per_tile = gsize // self.skip
        self.side = self.tcount * self.per_tile // 2
        self.ktiles = -(-ncoef // LANES)
        self.ht = -(-self.ktiles // 2)
        self.ht += -self.ht % GROUPS
        self.gt = self.ht // GROUPS
        self.nh = min(self.side, self.ht)
        self.pieces = [(j * self.ht // self.nh, (j + 1) * self.ht // self.nh) for j in range(self.nh)]
        self.sizes = sorted({b - a for a, b in self.pieces})
        self.largest = max(self.sizes)
        self.width = 2 * self.ht * LANES


def kernel(
    cfg,
    basis_hbm, pid_hbm, bid_hbm, mag_hbm, ivar_hbm,
    out_ref,
    bas, pid, bid, mag, ivar,
    bhi, blo, thi, tlo, cnt, wgt,
    snd, loc, rsb, agb,
    in_sems, send_sems, rs_sems, ag_sems,
):
    pixels, ncoef, objs, plan = cfg
    ht, gt, nh = plan.ht, plan.gt, plan.nh
    ndev, tsize, gsize = plan.ndev, plan.tsize, plan.gsize
    total_pix = pixels * ndev
    hrows = ht * LANES
    grows = gt * LANES

    tile = lax.axis_index("tile")
    grp = lax.axis_index("grp")
    me = tile * gsize + grp
    inside = (tile >= plan.t0) & (tile < plan.t0 + plan.tcount) & (lax.rem(grp, plan.skip) == plan.odd)
    k = (tile - plan.t0) * plan.per_tile + grp // plan.skip
    my_half = k // plan.side
    my_piece = k - my_half * plan.side
    is_owner = inside & (my_piece < nh)
    low = tile < tsize // 2
    near = jnp.where(low, 0, 1)
    far = 1 - near
    same = lax.rem(tile, GROUPS)
    other = 1 - same

    def at(t, g):
        return {"tile": t, "grp": g}

    def owner_place(h, j):
        o = h * plan.side + j
        return plan.t0 + o // plan.per_tile, lax.rem(o, plan.per_tile) * plan.skip + plan.odd

    barrier = pltpu.get_barrier_semaphore()

    def steps(n, shift):
        return min(shift, n - shift)

    def reach(move):
        a, b = move
        outer, inner = (a // 2, a % 2) if tsize % 2 == 0 else (a, 0)
        return -(
            steps(max(tsize // 2, 1), outer) + inner
            + steps(max(gsize // 2, 1), (b + 1) // 2 % max(gsize // 2, 1)) * 1.5 + (b % 2) * 0.95
        )

    def toward(a, b):
        g = lax.rem(grp + b, gsize)
        if tsize % 2:
            return lax.rem(tile + a, tsize), g
        outer = lax.rem(tile // 2 + a // 2, tsize // 2)
        return outer * 2 + lax.rem(tile + a % 2, 2), g

    def everyone(send):
        moves = sorted(((a, b) for a in range(tsize) for b in range(gsize) if a or b), key=reach)
        if ndev - 1 <= UNROLL:
            for a, b in moves:
                send(*toward(a, b))
        else:
            def some(i, _):
                a = lax.rem(i // gsize + tsize // 2, tsize)
                b = lax.rem(i, gsize)

                @pl.when(i != (tsize - tsize // 2) * gsize)
                def _():
                    send(lax.rem(tile + a, tsize), lax.rem(grp + b, gsize))
                return 0

            lax.fori_loop(0, ndev, some, 0)

    small = []
    for i, (src, dst) in enumerate(((pid_hbm, pid), (bid_hbm, bid), (mag_hbm, mag), (ivar_hbm, ivar))):
        c = pltpu.make_async_copy(src, dst, in_sems.at[i])
        c.start()
        small.append(c)

    chunks = []
    for c in range(2 * GROUPS):
        a, z = c * grows, min((c + 1) * grows, ncoef)
        rows = pl.ds(a, z - a)
        chunks.append((a, z, pltpu.make_async_copy(basis_hbm.at[rows, :], bas.at[rows, :], in_sems.at[4 + c])))
    low_order = list(range(GROUPS, 2 * GROUPS)) + list(range(GROUPS))
    high_order = list(range(2 * GROUPS))

    @pl.when(low)
    def _():
        for c in low_order:
            chunks[c][2].start()

    @pl.when(jnp.logical_not(low))
    def _():
        for c in high_order:
            chunks[c][2].start()

    @pl.when(is_owner)
    def _():
        everyone(
            lambda t, g: pl.semaphore_signal(barrier, inc=1, device_id=at(t, g), device_id_type=MESH)
        )

    cnt[...] = jnp.zeros_like(cnt)
    wgt[...] = jnp.zeros_like(wgt)
    agb[...] = jnp.zeros_like(agb)

    for c in small:
        c.wait()
    blocks = pixels // LANES
    keys = -(-BANDS * blocks // 8) * 8
    orow = objs // LANES
    step_rows = 8 if orow % 8 == 0 else 1

    def histogram(dst, value_of):
        def hist_step(i, acc):
            lhs_parts, rhs_parts = [], []
            for r in range(step_rows):
                here = pl.ds(i * step_rows + r, 1)
                pix = pid[here, :]
                key = bid[here, :] * blocks + pix // LANES
                lane = lax.rem(pix, LANES)
                hot = lax.broadcasted_iota(jnp.int32, (LANES, LANES), 0) == lane
                rhs_parts.append(jnp.where(hot, F32(1), F32(0)).astype(F8))
                sel = lax.broadcasted_iota(jnp.int32, (keys, LANES), 0) == key
                value = value_of(here)
                high = value.astype(BF16).astype(F32)
                lhs_parts.append(
                    jnp.concatenate(
                        [jnp.where(sel, x, F32(0)) for x in (high, value - high)], axis=0
                    ).astype(BF16)
                )
            lhs = jnp.concatenate(lhs_parts, axis=1)
            rhs = jnp.concatenate(rhs_parts, axis=1)
            return acc + lax.dot_general(
                lhs, rhs, (((1,), (1,)), ((), ())), preferred_element_type=F32
            )

        acc = lax.fori_loop(
            0, orow // step_rows, hist_step, jnp.zeros((2 * keys, LANES), F32), unroll=4
        )
        both = acc[:keys] + acc[keys:]
        for b in range(BANDS):
            for j in range(blocks):
                r = b * blocks + j
                dst[b : b + 1, j * LANES : (j + 1) * LANES] = both[r : r + 1]

    histogram(wgt, lambda here: ivar[here, :] * mag[here, :])

    def halve(rows, x):
        h = x.astype(BF16)
        bhi[rows, :] = h
        blo[rows, :] = ((x - h.astype(F32)) * SHIFT).astype(F8)

    def halve_rows(a, z):
        full = (z - a) // SUB

        for i in range(a, a + full * SUB, SUB):
            halve(slice(i, i + SUB), bas[i : i + SUB, :])

        done = a + full * SUB
        if done < z:
            pad = jnp.zeros((SUB - (z - done), pixels), F32)
            halve(slice(done, done + SUB), jnp.concatenate([bas[done:z, :], pad], axis=0))

    for z in range(-(-ncoef // SUB) * SUB, plan.width, SUB):
        halve(slice(z, z + SUB), jnp.zeros((SUB, pixels), F32))

    def to_coef(s, lhs, base, first, count):
        dims = (((1,), (1,)), ((), ()))
        for a in range(0, count, 2):
            n = min(2, count - a)
            start = (first + a) * LANES
            if not isinstance(start, int):
                start = pl.multiple_of(start, LANES)
            rows = pl.ds(start, n * LANES)
            part = fold(
                lax.dot_general(lhs[0], bhi[rows, :], dims, preferred_element_type=F32)
                + lax.dot_general(lhs[1], blo[rows, :], dims, preferred_element_type=F32)
            )
            for i in range(n):
                snd[s, base + a + i] = part[:, i * LANES : (i + 1) * LANES]

    def send_group(s, h, group):
        across = grp // plan.skip
        todo = list(enumerate(plan.pieces[: nh // GROUPS]))
        for turn in (0, 1) if len(todo) == 2 else (None,):
            for j, (a, z) in todo:
                t, g = owner_place(h, group * (nh // GROUPS) + j)
                other_device = jnp.logical_not((t == tile) & (g == grp))
                if turn is not None:
                    other_device = other_device & ((across != j) if turn == 0 else (across == j))

                @pl.when(other_device)
                def _():
                    pltpu.make_async_remote_copy(
                        src_ref=snd.at[s, pl.ds(h * ht + group * gt + a, z - a), pl.ds(0, BANDS)],
                        dst_ref=rsb.at[s, me, pl.ds(0, z - a), pl.ds(0, BANDS)],
                        send_sem=send_sems.at[s, 0], recv_sem=rs_sems.at[s],
                        device_id=at(t, g), device_id_type=MESH,
                    ).start()

    def landed(part, sem):
        pltpu.make_async_copy(part, part, sem).wait()

    def turn_basis():
        @pl.loop(0, 2 * ht)
        def _(i):
            rows = pl.ds(pl.multiple_of(i * LANES, LANES), LANES)
            for c in range(0, pixels, LANES):
                thi[c : c + LANES, rows] = bhi[rows, c : c + LANES].T
                tlo[c : c + LANES, rows] = blo[rows, c : c + LANES].T

    def produce(s, scaled, settle):
        lhs = split_rows(scaled)
        for h, g in ((far, other), (far, same), (near, other), (near, same)):
            base = h * ht + g * gt
            for a in range(0, gt, 2):
                n = min(2, gt - a)
                cols = pl.ds(pl.multiple_of((base + a) * LANES, LANES), n * LANES)
                part = fold(
                    jnp.dot(lhs[0], thi[:, cols], preferred_element_type=F32)
                    + jnp.dot(lhs[1], tlo[:, cols], preferred_element_type=F32)
                )
                for i in range(n):
                    settle(base + a + i, part[:, i * LANES : (i + 1) * LANES])
            send_group(s, h, g)

    def own(s):
        for n in plan.sizes:
            first = my_piece * ht // nh
            size = (my_piece + 1) * ht // nh - first

            @pl.when(is_owner & (size == n))
            def _():
                mine = pl.ds(my_half * ht + first, n)
                rsb[s, me, :n] = snd[s, mine]
                landed(rsb.at[s, pl.ds(0, ndev - 1), pl.ds(0, n), pl.ds(0, BANDS)], rs_sems.at[s])
                for i in range(n):
                    agb[s, my_half * ht + first + i, :BANDS] = tree(
                        [rsb[s, d, i, :BANDS] for d in range(ndev)]
                    )
                spread = agb.at[s, mine, pl.ds(0, BANDS)]
                group = first // gt

                def forward(t, g):
                    pltpu.make_async_remote_copy(
                        src_ref=spread, dst_ref=spread,
                        send_sem=send_sems.at[s, 1], recv_sem=ag_sems.at[s, my_half, group],
                        device_id=at(t, g), device_id_type=MESH,
                    ).start()

                everyone(forward)

    def group_wait(s, h, g):
        def part(m):
            return agb.at[s, pl.ds(0, m), pl.ds(0, BANDS)]

        sem = ag_sems.at[s, h, g]
        first = my_piece * ht // nh
        size = (my_piece + 1) * ht // nh - first
        holds = is_owner & (my_half == h) & (first // gt == g)

        @pl.when(jnp.logical_not(holds))
        def _():
            landed(part(gt), sem)

        for n in plan.sizes:
            if n < gt:
                @pl.when(holds & (size == n))
                def _():
                    landed(part(gt - n), sem)

    def consume(s, project):
        quarters, pix = [], []
        for h, g in ((near, same), (near, other), (far, same), (far, other)):
            group_wait(s, h, g)
            here = jnp.concatenate([agb[s, h * ht + g * gt + i] for i in range(gt)], axis=1)
            quarters.append(here)
            if project:
                lhs = split_rows(here)
                rows = pl.ds(pl.multiple_of((h * GROUPS + g) * grows, LANES), grows)
                pix.append(
                    jnp.dot(lhs[0], bhi[rows, :], preferred_element_type=F32)
                    + jnp.dot(lhs[1], blo[rows, :], preferred_element_type=F32)
                )
        total = None
        if project:
            for part in pix:
                total = part if total is None else total + part
            total = fold(total)
        return quarters, total

    def dot_all(xs, ys):
        both = sum(jnp.sum(x * y, axis=0, keepdims=True) for x, y in zip(xs, ys))
        return jnp.sum(both, axis=1, keepdims=True)

    right_lhs = split_rows(wgt[...])

    def opening(order):
        def ready(c):
            a, z, copy = chunks[c]
            copy.wait()
            halve_rows(a, z)

        ready(order[0])
        for i, c in enumerate(order):
            h = c // GROUPS
            if i + 1 < len(order):
                ready(order[i + 1])
            to_coef(0, right_lhs, c * gt, c * gt, gt)
            if i == 0:
                pl.semaphore_wait(barrier, waited)
            send_group(0, h, c % GROUPS)

    waited = jnp.where(is_owner, 2 * nh - 1, 2 * nh)

    @pl.when(low)
    def _():
        opening(low_order)

    @pl.when(jnp.logical_not(low))
    def _():
        opening(high_order)

    turn_basis()
    own(0)
    histogram(cnt, lambda here: ivar[here, :])
    sums, seen = consume(0, True)
    scale = 1 / jnp.sqrt(F32(total_pix))
    mean = F32(1 / total_pix)
    residual = [x * scale for x in sums]
    direction = residual
    answer = [jnp.zeros_like(x) for x in residual]
    norm_now = dot_all(residual, residual)

    def first_settle(t, part):
        here = part * scale
        loc[t] = here
        snd[1, t] = here

    settle = first_settle
    for it in range(ITERS):
        last = it + 1 == ITERS
        produce(it + 1, cnt[...] * seen, settle)
        own(it + 1)
        sums, seen = consume(it + 1, not last)
        image = [x * mean + RIDGE * d for x, d in zip(sums, direction)]
        step_len = norm_now / dot_all(direction, image)
        answer = [x + step_len * d for x, d in zip(answer, direction)]
        residual = [x - step_len * y for x, y in zip(residual, image)]
        if not last:
            norm_next = dot_all(residual, residual)
            rate = norm_next / norm_now
            direction = [x + rate * d for x, d in zip(residual, direction)]
            norm_now = norm_next

            def settle(t, part, s=it + 1, step_len=step_len, rate=rate):
                old = snd[s, t]
                here = loc[t] - step_len * (part * mean + RIDGE * old)
                loc[t] = here
                snd[s + 1, t] = here + rate * old

    def swap(flag, x, y):
        return jnp.where(flag, x, y), jnp.where(flag, y, x)

    def ordered(quarters):
        first = swap(same == 0, *quarters[:2])
        second = swap(same == 0, *quarters[2:])
        pairs = [swap(low, x, y) for x, y in zip(first, second)]
        return jnp.concatenate([pairs[0][0], pairs[1][0], pairs[0][1], pairs[1][1]], axis=1)

    out_ref[0] = ordered(answer)[:, : plan.ktiles * LANES]
    out_ref[1] = ordered(residual)[:, : plan.ktiles * LANES]

    first = my_piece * ht // nh
    size = (my_piece + 1) * ht // nh - first
    for n in plan.sizes:
        @pl.when(is_owner & (size == n))
        def _():
            for s in range(STEPS):
                landed(snd.at[s, pl.ds(0, 2 * ht - n), pl.ds(0, BANDS)], send_sems.at[s, 0])
                landed(rsb.at[s, pl.ds(0, ndev - 1), pl.ds(0, n), pl.ds(0, BANDS)], send_sems.at[s, 1])

    @pl.when(jnp.logical_not(is_owner))
    def _():
        for s in range(STEPS):
            landed(snd.at[s, pl.ds(0, 2 * ht), pl.ds(0, BANDS)], send_sems.at[s, 0])


def body(basis, pixel_ids, band_ids, mags, inv_var):
    pixels, ncoef = basis.shape
    objs = pixel_ids.shape[0]
    plan = Plan(lax.axis_size("tile"), lax.axis_size("grp"), ncoef)
    cfg = (pixels, ncoef, objs, plan)
    fold_objs = lambda x: x.reshape(objs // LANES, LANES)
    anyspec = pl.BlockSpec(memory_space=pl.ANY)
    out = jax.ShapeDtypeStruct((2, 8, plan.ktiles * LANES), F32)
    orow = objs // LANES
    both = pl.pallas_call(
        functools.partial(kernel, cfg),
        out_shape=out,
        in_specs=[anyspec] * 5,
        out_specs=pl.BlockSpec(memory_space=pltpu.VMEM),
        scratch_shapes=[
            pltpu.VMEM((ncoef, pixels), F32),
            pltpu.VMEM((orow, LANES), jnp.int32),
            pltpu.VMEM((orow, LANES), jnp.int32),
            pltpu.VMEM((orow, LANES), F32),
            pltpu.VMEM((orow, LANES), F32),
            pltpu.VMEM((plan.width, pixels), BF16),
            pltpu.VMEM((plan.width, pixels), F8),
            pltpu.VMEM((pixels, plan.width), BF16),
            pltpu.VMEM((pixels, plan.width), F8),
            pltpu.VMEM((8, pixels), F32),
            pltpu.VMEM((8, pixels), F32),
            pltpu.VMEM((STEPS, 2 * plan.ht, 8, LANES), F32),
            pltpu.VMEM((2 * plan.ht, 8, LANES), F32),
            pltpu.VMEM((STEPS, plan.ndev, plan.largest, 8, LANES), F32),
            pltpu.VMEM((STEPS, 2 * plan.ht, 8, LANES), F32),
            pltpu.SemaphoreType.DMA((4 + 2 * GROUPS,)),
            pltpu.SemaphoreType.DMA((STEPS, 2)),
            pltpu.SemaphoreType.DMA((STEPS,)),
            pltpu.SemaphoreType.DMA((STEPS, 2, GROUPS)),
        ],
        compiler_params=pltpu.CompilerParams(collective_id=0, has_side_effects=True),
    )(basis.T, fold_objs(pixel_ids), fold_objs(band_ids), fold_objs(mags), fold_objs(inv_var))
    return both[0, :BANDS, :ncoef], both[1, :BANDS, :ncoef]


def solution(mesh):
    placed = (
        P(("tile", "grp"), None),
        P(("tile", "grp")),
        P(("tile", "grp")),
        P(("tile", "grp")),
        P(("tile", "grp")),
    )
    return jax.shard_map(body, mesh=mesh, in_specs=placed, out_specs=(P(), P()), check_vma=False)
```
